32 devices in a mesh: fsdp: 8 (over y, x, core), seq: 4 (over z).
Axes of the slice: x: 2, y: 2, z: 4, core: 2. Of those that a mesh axis runs over, the one named last changes fastest.
Arguments:
- tokens: bfloat16 [8192, 2304], P('fsdp', 'seq'), may hold values from -70 to 70
- gain: float32 [2304], replicated, may hold values from 0.1 to 1.9
- w_query: bfloat16 [2304, 4096], P('fsdp', 'seq'), may hold values from -3 to 3
- w_key: bfloat16 [2304, 2048], P('fsdp', 'seq'), may hold values from -3 to 3
- w_value: bfloat16 [2304, 2048], P('fsdp', 'seq'), may hold values from -0.125 to 0.125
Outputs:
- context: bfloat16 [8192, 4096], P('fsdp', 'seq')
The draws below stay inside these ranges and needn't reach their ends.
All inputs are finite; a program needn't handle non-finite values.
Results may differ from the reference program's by a relative error of at most 0.012.
The reference program's roundings to bfloat16 on the way (of `normed`, `values` and `weights`) count: a program that leaves them out, or rounds other values in their place, can miss the bound.
Values may be sent and summed in bfloat16 or wider, within the bound.
A program may use at most 64 MiB of HBM per device.

```python
import math
import jax
import jax.numpy as jnp
from jax import lax

D = 2304
HEADS = 32
KV_HEADS = 16
HEAD_DIM = 128
SEQ_LEN = 1024
SEQS = 8


def draw_tokens(key, part):
    base_key, row_key, col_key = jax.random.split(jax.random.fold_in(key, 7), 3)
    count = SEQS * SEQ_LEN
    position = jnp.arange(D, dtype=jnp.float32) / D
    spread = math.log(10.0) * 0.5
    row_scale = jnp.exp(jax.random.uniform(row_key, (count, 1), jnp.float32, -spread, spread))
    col_scale = jnp.exp(jax.random.uniform(col_key, (1, D), jnp.float32, -spread, spread))
    base = jax.random.truncated_normal(base_key, -4.0, 4.0, (count, D), jnp.float32)
    ramp = jnp.exp(0.5 * math.log(3.0) * position)
    return (base * row_scale * col_scale * ramp[None, :]).astype(jnp.bfloat16)


def draw_w_query(key, part):
    base_key, scale_key = jax.random.split(jax.random.fold_in(key, 101))
    base = jax.random.truncated_normal(base_key, -4.0, 4.0, (D, HEADS * HEAD_DIM), jnp.float32)
    log_scale = jax.random.uniform(scale_key, (HEADS,), jnp.float32, 0.0, math.log(6.0))
    column_scale = jnp.repeat(jnp.exp(log_scale), HEAD_DIM)
    return (base * column_scale[None, :] / math.sqrt(D)).astype(jnp.bfloat16)


def draw_w_key(key, part):
    base_key, scale_key = jax.random.split(jax.random.fold_in(key, 202))
    base = jax.random.truncated_normal(base_key, -4.0, 4.0, (D, KV_HEADS * HEAD_DIM), jnp.float32)
    log_scale = jax.random.uniform(scale_key, (KV_HEADS,), jnp.float32, 0.0, math.log(6.0))
    column_scale = jnp.repeat(jnp.exp(log_scale), HEAD_DIM)
    return (base * column_scale[None, :] / math.sqrt(D)).astype(jnp.bfloat16)


def steps_of(own_key, shape, shards, least, top_value):
    def one(dim, blocks):
        heights = jax.random.uniform(jax.random.fold_in(jax.random.fold_in(own_key, 6), dim), (blocks,), jnp.float32, least / len(shards), top_value / len(shards))
        return jnp.repeat(jnp.exp(heights), shape[dim] // blocks).reshape((-1,) + (1,) * (len(shape) - dim - 1))

    loudness = one(*shards[0])
    for cut in shards[1:]:
        loudness = loudness * one(*cut)
    return loudness


def gaussian(rng, extent, scale, bound, cuts=(), held_as=jnp.bfloat16):
    values = scale * jax.random.normal(rng, extent, jnp.float32)
    if cuts:
        values = values * steps_of(rng, extent, cuts, -0.22, 0.18)
    return jnp.clip(values, -bound, bound).astype(held_as)


def setup_inputs(seed: int = 0) -> dict:
    arg_keys = jax.random.split(jax.random.key(seed), 6)
    return {
        "tokens": draw_tokens(jax.random.fold_in(arg_keys[5], 71), 0),
        "gain": jnp.clip(1.0 + 0.18 * jax.random.normal(arg_keys[1], (D,), jnp.float32), 0.1, 1.9),
        "w_query": draw_w_query(jax.random.fold_in(arg_keys[5], 71), 0),
        "w_key": draw_w_key(jax.random.fold_in(arg_keys[5], 71), 0),
        "w_value": gaussian(arg_keys[4], (D, KV_HEADS * HEAD_DIM), D ** -0.5, 0.125, ((0, 8), (1, 4))),
    }


def rotate(values, positions):
    half = values.shape[-1] // 2
    index = jnp.arange(half, dtype=jnp.float32)
    freqs = jnp.power(jnp.float32(10000.0), -2.0 * index / values.shape[-1])
    angle = positions[:, None] * freqs[None, :]
    cosine = jnp.cos(angle)[:, None, :]
    sine = jnp.sin(angle)[:, None, :]
    first = values[..., :half]
    second = values[..., half:]
    return jnp.concatenate([first * cosine - second * sine, second * cosine + first * sine], axis=-1)

def one_sequence(rows, gain, w_query, w_key, w_value):
    length = rows.shape[0]
    groups = HEADS // KV_HEADS
    floats = rows.astype(jnp.float32)
    inv_rms = lax.rsqrt(lax.optimization_barrier(jnp.mean(floats * floats, axis=-1, keepdims=True)) + 1e-06)
    normed = (floats * inv_rms * gain[None, :]).astype(jnp.bfloat16)
    positions = jnp.arange(length, dtype=jnp.float32)
    query_raw = jnp.dot(normed, w_query, preferred_element_type=jnp.float32).reshape(length, HEADS, HEAD_DIM)
    key_raw = jnp.dot(normed, w_key, preferred_element_type=jnp.float32).reshape(length, KV_HEADS, HEAD_DIM)
    values = jnp.dot(normed, w_value, preferred_element_type=jnp.float32).astype(jnp.bfloat16).reshape(length, KV_HEADS, HEAD_DIM)
    query = rotate(query_raw, positions).astype(jnp.bfloat16).reshape(length, KV_HEADS, groups, HEAD_DIM)
    keys = rotate(key_raw, positions).astype(jnp.bfloat16)
    scale = 1.0 / jnp.sqrt(jnp.float32(144.0))
    scores = jnp.einsum('lgqd,mgd->gqlm', query.astype(jnp.float32), keys.astype(jnp.float32)) * scale
    capped = 50.0 * jnp.tanh(scores / 50.0)
    causal = jnp.arange(length)[None, :] <= jnp.arange(length)[:, None]
    expo = jnp.where(causal[None, None], jnp.exp(capped), 0.0)
    weights = (expo / lax.optimization_barrier(jnp.sum(expo, axis=-1, keepdims=True))).astype(jnp.bfloat16)
    context = jnp.einsum('gqlm,mgd->lgqd', weights.astype(jnp.float32), values.astype(jnp.float32))
    return context.reshape(length, HEADS * HEAD_DIM).astype(jnp.bfloat16)

def reference(tokens, gain, w_query, w_key, w_value):
    seq_len = tokens.shape[0] // SEQS
    stacked = tokens.reshape(SEQS, seq_len, D)
    result = lax.map(lambda rows: one_sequence(rows, gain, w_query, w_key, w_value), stacked)
    return result.reshape(SEQS * seq_len, HEADS * HEAD_DIM)
```

```python
import functools
import math

import jax
import jax.numpy as jnp
import numpy as np
from jax import lax
from jax.experimental import pallas as pl
from jax.experimental.pallas import tpu as pltpu
from jax.sharding import PartitionSpec as P

HEAD_DIM = 128
ROWS = 256
WIRE = 128
MESH = pl.DeviceIdType.MESH


def kernel(
    n, kv, groups, chunks,
    tok_in, gain_in, cos_in, sin_in, wq_in, wk_in, wv_in, out_hbm,
    tok, w, nrm, q_s, k_s, v_s, acc, gain_ref, cos_ref, sin_ref, part_ref, ss,
    tok_sem, local_sem, t_send, t_recv, w_send, w_recv, s_send, s_recv,
):
    z = lax.axis_index("seq")
    me = lax.axis_index("fsdp")
    core = lax.rem(me, 2)
    xpos = lax.rem(lax.div(me, 2), 2)
    ypos = lax.div(me, 4)
    mate = me + 1 - 2 * core
    xnbr = me + 2 - 4 * xpos
    ynbr = me + 4 - 8 * ypos
    diag = xnbr + 4 - 8 * ypos
    depth = wk_in.shape[0]
    width = wk_in.shape[1]
    cols = tok_in.shape[0]
    pieces = 2 + groups
    wire = tok_in.shape[1] // chunks

    def own_slot(first, size):
        rows = pl.ds(pl.multiple_of(z * cols, 16), cols)
        return tok.at[rows, pl.ds(first, size)]

    def load(first, size, i):
        return pltpu.make_async_copy(tok_in.at[:, pl.ds(first, size)], own_slot(first, size), tok_sem.at[i])

    loads = [load(0, wire, 0), load(wire, wire, 1), load(2 * wire, tok_in.shape[1] - 2 * wire, 2)]
    for copy in loads:
        copy.start()

    barrier = pltpu.get_barrier_semaphore()
    for other in (mate, xnbr, ynbr):
        pl.semaphore_signal(barrier, inc=1, device_id={"fsdp": other}, device_id_type=MESH)

    @pl.when(z > 0)
    def _():
        pl.semaphore_signal(barrier, inc=1, device_id={"seq": z - 1}, device_id_type=MESH)

    @pl.when(z < n - 1)
    def _():
        pl.semaphore_signal(barrier, inc=1, device_id={"seq": z + 1}, device_id_type=MESH)

    peers = 5 - jnp.where(z == 0, 1, 0) - jnp.where(z == n - 1, 1, 0)
    pl.semaphore_wait(barrier, peers)

    def w_own(p):
        if p == 0:
            return wk_in
        if p == 1:
            return wv_in
        return wq_in.at[:, pl.ds((p - 2) * width, width)]

    def w_slot(p, f):
        return w.at[p, pl.ds(pl.multiple_of(f * depth, 16), depth), :]

    def w_copy(p, kind, lane):
        shard = (me, xnbr, ynbr, diag)[kind]
        src = w_own(p) if kind == 0 else w_slot(p, shard)
        return pltpu.make_async_remote_copy(
            src_ref=src, dst_ref=w_slot(p, shard),
            send_sem=w_send.at[lane, kind, p], recv_sem=w_recv.at[shard, p],
            device_id={"fsdp": (mate, xnbr, ynbr)[lane]}, device_id_type=MESH,
        )

    def w_wait(p, shard):
        pltpu.make_async_copy(w_slot(p, shard), w_slot(p, shard), w_recv.at[shard, p]).wait()

    def t_slot(s, c):
        first = c * wire if isinstance(c, int) else pl.multiple_of(c * wire, wire)
        return tok.at[pl.ds(pl.multiple_of(s * cols, 16), cols), pl.ds(first, wire)]

    def t_copy(block, c, side):
        return pltpu.make_async_remote_copy(
            src_ref=t_slot(block, c), dst_ref=t_slot(block, c),
            send_sem=t_send.at[side, block, c], recv_sem=t_recv.at[block, c],
            device_id={"seq": z + 1 - 2 * side}, device_id_type=MESH,
        )

    def t_wait(block, c):
        pltpu.make_async_copy(t_slot(block, c), t_slot(block, c), t_recv.at[block, c]).wait()

    def own_tokens(c, do):
        @pl.when(z < n - 1)
        def _():
            do(t_copy(z, c, 0))

        @pl.when(z > 0)
        def _():
            do(t_copy(z, c, 1))

    def own_weights(do):
        for p in range(pieces):
            for lane in (1, 2, 0):
                do(w_copy(p, 0, lane))

    def start(copy):
        copy.start()

    def s_copy(block, side):
        return pltpu.make_async_remote_copy(
            src_ref=ss.at[block], dst_ref=ss.at[block],
            send_sem=s_send.at[side, block], recv_sem=s_recv.at[block],
            device_id={"seq": z + 1 - 2 * side}, device_id_type=MESH,
        )

    def s_wait(block):
        pltpu.make_async_copy(ss.at[block], ss.at[block], s_recv.at[block]).wait()

    def own_sums(do):
        @pl.when(z < n - 1)
        def _():
            do(s_copy(z, 0))

        @pl.when(z > 0)
        def _():
            do(s_copy(z, 1))

    def first_tokens():
        for c in range(2):
            loads[c].wait()
            own_tokens(c, start)

    first_tokens()

    own_weights(start)
    local = []
    for p in range(pieces):
        local.append(pltpu.make_async_copy(w_own(p), w_slot(p, me), local_sem.at[p]))
    local.append(pltpu.make_async_copy(gain_in, gain_ref.at[0], local_sem.at[pieces]))
    local.append(pltpu.make_async_copy(cos_in, cos_ref, local_sem.at[pieces + 1]))
    local.append(pltpu.make_async_copy(sin_in, sin_ref, local_sem.at[pieces + 2]))
    for copy in local:
        copy.start()
    v_s[:, :, HEAD_DIM:] = jnp.ones((kv, v_s.shape[1], HEAD_DIM), jnp.bfloat16)

    loads[2].wait()
    last = t_slot(z, chunks - 1)[...].astype(jnp.float32)
    ss[z] = jnp.sum(last * last, axis=0, keepdims=True)

    def relay(dist, c):
        @pl.when((z >= dist) & (z < n - 1))
        def _():
            t_wait(z - dist, c)
            t_copy(z - dist, c, 0).start()

        @pl.when((z + dist < n) & (z > 0))
        def _():
            t_wait(z + dist, c)
            t_copy(z + dist, c, 1).start()

    def relay_sums(dist):
        @pl.when((z >= dist) & (z < n - 1))
        def _():
            s_wait(z - dist)
            s_copy(z - dist, 0).start()

        @pl.when((z + dist < n) & (z > 0))
        def _():
            s_wait(z + dist)
            s_copy(z + dist, 1).start()

    def settle(dist, c):
        @pl.when((z >= dist) & (z == n - 1))
        def _():
            t_wait(z - dist, c)

        @pl.when((z + dist < n) & (z == 0))
        def _():
            t_wait(z + dist, c)

    def token_round(k):
        for dist in range(n - 2, 0, -1):
            c = k - dist + 1
            if 0 <= c < chunks:
                relay(dist, c)
        if k + 2 < chunks:
            own_tokens(k + 2, start)

    rounds = chunks + n - 3
    early = min(n + 2, rounds)
    for step in range(max(early, pieces)):
        if step < early:
            token_round(step)
        if step == 1:
            own_sums(start)
        if 2 <= step < n:
            relay_sums(step - 1)
        if step < pieces:
            w_wait(step, xnbr)
            w_copy(step, 1, 0).start()

            @pl.when(core == 1)
            def _():
                w_copy(step, 1, 2).start()

            w_wait(step, ynbr)
            w_copy(step, 2, 0).start()

            @pl.when(core == 0)
            def _():
                w_copy(step, 2, 1).start()

    for p in range(pieces):
        w_wait(p, diag)
        w_copy(p, 3, 0).start()
    for p in range(pieces):
        for shard in (mate, xnbr + 1 - 2 * core, ynbr + 1 - 2 * core, diag + 1 - 2 * core):
            w_wait(p, shard)
    for copy in local:
        copy.wait()

    scale = 1.0 / (12.0 * 50.0)
    peak = 50.0 * math.log2(math.e)

    R = wire

    def rotate_at(rows):
        cosine = cos_ref[rows, :]
        sine = sin_ref[rows, :]
        return lambda x: (x * cosine + pltpu.roll(x, HEAD_DIM // 2, 1) * sine).astype(jnp.bfloat16)

    def tail():
        length = chunks * wire
        first = length - R
        rows = pl.ds(first, R)
        near = (n - 1) * cols
        left = z == 0
        near_at = pl.ds(pl.multiple_of(jnp.where(left, 0, cols), 16), near)
        far_at = pl.ds(pl.multiple_of(jnp.where(left, near, 0), 16), cols)
        for dist in range(1, n):
            @pl.when(left)
            def _():
                s_wait(z + dist)

            @pl.when(z == n - 1)
            def _():
                s_wait(z - dist)

        for dist in range(1, n - 1):
            settle(dist, chunks - 1)
        total = ss[0]
        for s in range(1, n):
            total += ss[s]
        inv = lax.rsqrt(total / (n * cols) + 1e-06)
        inv = jnp.broadcast_to(inv, (R, R)).T[:, :1]
        gain = gain_ref[...]
        near_gain = jnp.where(left, gain[:, :near], gain[:, cols:])
        far_gain = jnp.where(left, gain[:, near:], gain[:, :cols])
        floats = tok[near_at, rows].T.astype(jnp.float32)
        normed = (floats * inv * near_gain).astype(jnp.bfloat16)
        for p in range(pieces):
            part_ref[p] = jnp.dot(normed, w[p, near_at, :], preferred_element_type=jnp.float32)
        settle(n - 1, chunks - 1)
        floats = tok[far_at, rows].T.astype(jnp.float32)
        normed = (floats * inv * far_gain).astype(jnp.bfloat16)
        turn = rotate_at(rows)

        def project(p):
            return part_ref[p] + jnp.dot(normed, w[p, far_at, :], preferred_element_type=jnp.float32)

        raw = project(0)
        for h in range(kv):
            k_s[h, rows, :] = turn(raw[:, h * HEAD_DIM : (h + 1) * HEAD_DIM])
        raw = project(1)
        for h in range(kv):
            v_s[h, rows, :HEAD_DIM] = raw[:, h * HEAD_DIM : (h + 1) * HEAD_DIM].astype(jnp.bfloat16)
        for g in range(groups):
            raw = project(2 + g)
            for i in range(kv):
                head = g * kv + i
                at = (head % groups) * R
                q_s[head // groups, at : at + R, :] = turn(raw[:, i * HEAD_DIM : (i + 1) * HEAD_DIM])
        row_id = lax.rem(lax.broadcasted_iota(jnp.int32, (groups * R, ROWS), 0), R)
        mask = lax.broadcasted_iota(jnp.int32, (groups * R, ROWS), 1) <= row_id + (ROWS - R)
        for h in range(kv):
            sums = None
            for low in range(0, length, ROWS):
                keys = pl.ds(low, ROWS)
                s = lax.dot_general(
                    q_s[h, : groups * R, :], k_s[h, keys, :], (((1,), (1,)), ((), ())),
                    preferred_element_type=jnp.float32,
                )
                e = jnp.exp2(jnp.tanh(s * scale) * peak)
                if low + ROWS == length:
                    e = jnp.where(mask, e, 0.0)
                e = jnp.dot(e.astype(jnp.bfloat16), v_s[h, keys, :], preferred_element_type=jnp.float32)
                sums = e if sums is None else sums + e
            for g in range(groups):
                head = h * groups + g
                part = sums[g * R : (g + 1) * R, :]
                out_hbm[rows, head * HEAD_DIM : (head + 1) * HEAD_DIM] = (
                    part[:, :HEAD_DIM] / part[:, HEAD_DIM:]
                ).astype(jnp.bfloat16)

    def chunk(first, low, last, base_count, part):
        rows = pl.ds(first, R)
        for dist in range(1, n):
            settle(dist, part)
        raw = tok[:, rows].T
        floats = raw.astype(jnp.float32)
        total = jnp.sum(floats * floats, axis=-1, keepdims=True)
        inv = lax.rsqrt(total / (n * cols) + 1e-06)
        nrm[:R, :] = (floats * inv * gain_ref[...]).astype(jnp.bfloat16)
        normed = nrm[:R, :]
        rotate = rotate_at(rows)

        raw = jnp.dot(normed, w[0], preferred_element_type=jnp.float32)
        for h in range(kv):
            k_s[h, rows, :] = rotate(raw[:, h * HEAD_DIM : (h + 1) * HEAD_DIM])
        raw = jnp.dot(normed, w[1], preferred_element_type=jnp.float32)
        for h in range(kv):
            v_s[h, rows, :HEAD_DIM] = raw[:, h * HEAD_DIM : (h + 1) * HEAD_DIM].astype(jnp.bfloat16)
        for g in range(groups):
            raw = jnp.dot(normed, w[2 + g], preferred_element_type=jnp.float32)
            for i in range(kv):
                head = g * kv + i
                at = (head % groups) * R
                q_s[head // groups, at : at + R, :] = rotate(
                    raw[:, i * HEAD_DIM : (i + 1) * HEAD_DIM]
                )

        def block(h, keys, mask):
            s = lax.dot_general(
                q_s[h, : groups * R, :], k_s[h, keys, :], (((1,), (1,)), ((), ())),
                preferred_element_type=jnp.float32,
            )
            e = jnp.exp2(jnp.tanh(s * scale) * peak)
            if mask is not None:
                e = jnp.where(mask, e, 0.0)
            return jnp.dot(
                e.astype(jnp.bfloat16), v_s[h, keys, :], preferred_element_type=jnp.float32
            )

        row_id = lax.rem(lax.broadcasted_iota(jnp.int32, (groups * R, last), 0), R)
        mask = lax.broadcasted_iota(jnp.int32, (groups * R, last), 1) <= row_id + (last - R)
        top = pl.ds(low, last)
        for h in range(kv):
            acc[h, : groups * R, :] = block(h, top, mask)

        def inner(j, carry):
            keys = pl.ds(pl.multiple_of(j * ROWS, ROWS), ROWS)
            for h in range(kv):
                acc[h, : groups * R, :] += block(h, keys, None)
            return carry

        lax.fori_loop(0, base_count, inner, 0)
        for h in range(kv):
            for g in range(groups):
                sums = acc[h, g * R : (g + 1) * R, :]
                head = h * groups + g
                out_hbm[rows, head * HEAD_DIM : (head + 1) * HEAD_DIM] = (
                    sums[:, :HEAD_DIM] / sums[:, HEAD_DIM:]
                ).astype(jnp.bfloat16)

    def body(c, carry):
        @pl.when(c == 0)
        def _():
            if early < rounds:
                token_round(early)

        @pl.when(c == 1)
        def _():
            for k in range(early + 1, rounds):
                token_round(k)

        low = pl.multiple_of(c * ROWS, ROWS)
        per = ROWS // R
        for i in range(per):
            first = pl.multiple_of(c * ROWS + i * R, R)
            part = c * per + i
            if i < per - 1:
                chunk(first, low, (i + 1) * R, c, part)
            else:
                @pl.when((part < chunks - 1) | ((z > 0) & (z < n - 1)))
                def _():
                    chunk(first, low, (i + 1) * R, c, part)
        return carry

    lax.fori_loop(0, chunks * wire // ROWS, body, 0)

    @pl.when((z == 0) | (z == n - 1))
    def _():
        tail()


    own_sums(lambda copy: copy.wait_send())
    for dist in range(1, n - 1):
        @pl.when((z >= dist) & (z < n - 1))
        def _():
            s_copy(z - dist, 0).wait_send()

        @pl.when((z + dist < n) & (z > 0))
        def _():
            s_copy(z + dist, 1).wait_send()

    own_weights(lambda copy: copy.wait_send())
    for c in range(chunks):
        own_tokens(c, lambda copy: copy.wait_send())
        for dist in range(1, n - 1):
            @pl.when((z >= dist) & (z < n - 1))
            def _():
                t_copy(z - dist, c, 0).wait_send()

            @pl.when((z + dist < n) & (z > 0))
            def _():
                t_copy(z + dist, c, 1).wait_send()

    for p in range(pieces):
        for kind in (1, 2, 3):
            w_copy(p, kind, 0).wait_send()

        @pl.when(core == 1)
        def _():
            w_copy(p, 1, 2).wait_send()

        @pl.when(core == 0)
        def _():
            w_copy(p, 2, 1).wait_send()


def fused(n, fsdp, tokens, gain, w_query, w_key, w_value):
    length, cols = tokens.shape
    depth, width = w_key.shape
    kv = width // HEAD_DIM
    groups = w_query.shape[1] // width
    chunks = length // WIRE
    half = HEAD_DIM // 2
    freqs = 10000.0 ** (-2.0 * np.arange(half) / HEAD_DIM)
    angle = np.arange(length)[:, None] * freqs[None, :]
    cosine = np.concatenate([np.cos(angle)] * 2, axis=1).astype(np.float32)
    sine = np.concatenate([-np.sin(angle), np.sin(angle)], axis=1).astype(np.float32)
    hbm = pl.BlockSpec(memory_space=pl.ANY)
    pieces = 2 + groups
    flops = 2 * length * fsdp * depth * width * pieces
    return pl.pallas_call(
        functools.partial(kernel, n, kv, groups, chunks),
        out_shape=pltpu.VMEM((length, w_query.shape[1]), jnp.bfloat16),
        in_specs=[hbm] * 7,
        out_specs=pl.BlockSpec(memory_space=pltpu.VMEM),
        scratch_shapes=[
            pltpu.VMEM((n * cols, length), jnp.bfloat16),
            pltpu.VMEM((pieces, fsdp * depth, width), jnp.bfloat16),
            pltpu.VMEM((WIRE, n * cols), jnp.bfloat16),
            pltpu.VMEM((kv, groups * WIRE, HEAD_DIM), jnp.bfloat16),
            pltpu.VMEM((kv, length, HEAD_DIM), jnp.bfloat16),
            pltpu.VMEM((kv, length, 2 * HEAD_DIM), jnp.bfloat16),
            pltpu.VMEM((kv, groups * WIRE, 2 * HEAD_DIM), jnp.float32),
            pltpu.VMEM((1, n * cols), jnp.float32),
            pltpu.VMEM((length, HEAD_DIM), jnp.float32),
            pltpu.VMEM((length, HEAD_DIM), jnp.float32),
            pltpu.VMEM((pieces, WIRE, width), jnp.float32),
            pltpu.VMEM((n, 1, WIRE), jnp.float32),
            pltpu.SemaphoreType.DMA((3,)),
            pltpu.SemaphoreType.DMA((3 + pieces,)),
            pltpu.SemaphoreType.DMA((2, n, chunks)),
            pltpu.SemaphoreType.DMA((n, chunks)),
            pltpu.SemaphoreType.DMA((3, 4, pieces)),
            pltpu.SemaphoreType.DMA((fsdp, pieces)),
            pltpu.SemaphoreType.DMA((2, n)),
            pltpu.SemaphoreType.DMA((n,)),
        ],
        compiler_params=pltpu.CompilerParams(
            collective_id=0, has_side_effects=True, vmem_limit_bytes=60 * 1024 * 1024
        ),
        cost_estimate=pl.CostEstimate(flops=flops, bytes_accessed=2 * length * cols, transcendentals=0),
    )(tokens.T, gain, jnp.asarray(cosine), jnp.asarray(sine), w_query, w_key, w_value)


def rotate(values, positions):
    half = values.shape[-1] // 2
    index = jnp.arange(half, dtype=jnp.float32)
    freqs = jnp.power(jnp.float32(10000.0), -2.0 * index / values.shape[-1])
    angle = positions[:, None] * freqs[None, :]
    cosine = jnp.cos(angle)[:, None, :]
    sine = jnp.sin(angle)[:, None, :]
    first = values[..., :half]
    second = values[..., half:]
    return jnp.concatenate(
        [first * cosine - second * sine, second * cosine + first * sine], axis=-1
    )


def local(tokens, gain, w_query, w_key, w_value):
    features = gain.shape[0]
    floats = tokens.astype(jnp.float32)
    square_sum = lax.psum(jnp.sum(floats * floats, axis=-1), "seq")
    inv_rms = lax.rsqrt(square_sum / features + 1e-06)[:, None]
    own_cols = tokens.shape[1]
    gain_part = lax.dynamic_slice_in_dim(gain, lax.axis_index("seq") * own_cols, own_cols, 0)
    own_normed = (floats * inv_rms * gain_part[None, :]).astype(jnp.bfloat16)
    normed = lax.all_gather(own_normed, "seq", axis=1, tiled=True)
    length = normed.shape[0]

    def add_one(piece):
        return jnp.dot(normed, piece, preferred_element_type=jnp.float32)

    query_raw = add_one(lax.all_gather(w_query, "fsdp", axis=0, tiled=True))
    key_raw = add_one(lax.all_gather(w_key, "fsdp", axis=0, tiled=True))
    value_raw = add_one(lax.all_gather(w_value, "fsdp", axis=0, tiled=True))
    local_heads = w_query.shape[1] // HEAD_DIM
    local_kv = w_key.shape[1] // HEAD_DIM
    groups = local_heads // local_kv
    positions = jnp.arange(length, dtype=jnp.float32)
    values = value_raw.astype(jnp.bfloat16).reshape(length, local_kv, HEAD_DIM)
    query = rotate(query_raw.reshape(length, local_heads, HEAD_DIM), positions).astype(jnp.bfloat16)
    query = query.reshape(length, local_kv, groups, HEAD_DIM)
    keys = rotate(key_raw.reshape(length, local_kv, HEAD_DIM), positions).astype(jnp.bfloat16)
    scale = 1.0 / jnp.sqrt(jnp.float32(144.0))
    block_rows = 512
    outputs = []
    for first_row in range(0, length, block_rows):
        extent = first_row + block_rows
        query_block = query[first_row:extent]
        scores = (
            jnp.einsum(
                "lgqd,mgd->gqlm", query_block, keys[:extent], preferred_element_type=jnp.float32
            )
            * scale
        )
        capped = 50.0 * jnp.tanh(scores / 50.0)
        causal = jnp.arange(extent)[None, :] <= (first_row + jnp.arange(block_rows))[:, None]
        exponent = jnp.where(causal[None, None], jnp.exp(capped), 0.0)
        weights = (exponent / jnp.sum(exponent, axis=-1, keepdims=True)).astype(jnp.bfloat16)
        context = jnp.einsum(
            "gqlm,mgd->lgqd", weights, values[:extent], preferred_element_type=jnp.float32
        )
        outputs.append(context.reshape(block_rows, local_heads * HEAD_DIM).astype(jnp.bfloat16))
    return jnp.concatenate(outputs, axis=0)


def solution(mesh):
    n, fsdp = mesh.shape["seq"], mesh.shape["fsdp"]
    in_specs = (P("fsdp", "seq"), P(), P("fsdp", "seq"), P("fsdp", "seq"), P("fsdp", "seq"))
    out_specs = P("fsdp", "seq")

    def step(tokens, gain, w_query, w_key, w_value):
        fits = (
            fsdp == 8
            and n == 4
            and tokens.shape[1] % 16 == 0
            and tokens.shape[0] % ROWS == 0
            and tokens.shape[0] >= 3 * ROWS
            and w_key.shape[0] % 16 == 0
            and w_query.shape[1] % w_key.shape[1] == 0
        )
        if fits:
            return fused(n, fsdp, tokens, gain, w_query, w_key, w_value)
        return local(tokens, gain, w_query, w_key, w_value)

    return jax.shard_map(step, mesh=mesh, in_specs=in_specs, out_specs=out_specs, check_vma=False)
```

```python
import functools
import math

import jax
import jax.numpy as jnp
import numpy as np
from jax import lax
from jax.experimental import pallas as pl
from jax.experimental.pallas import tpu as pltpu
from jax.sharding import PartitionSpec as P

HEAD_DIM = 128
ROWS = 256
WIRE = 128
LATE = 256
MESH = pl.DeviceIdType.MESH


def kernel(
    n, kv, groups, chunks,
    tok_in, gain_in, cos_in, sin_in, wq_in, wk_in, wv_in, out_hbm,
    tok, w, nrm, q_s, k_s, v_s, acc, gain_ref, cos_ref, sin_ref, part_ref, ss,
    tok_sem, local_sem, t_send, t_recv, w_send, w_recv, s_send, s_recv,
):
    z = lax.axis_index("seq")
    me = lax.axis_index("fsdp")
    core = lax.rem(me, 2)
    xpos = lax.rem(lax.div(me, 2), 2)
    ypos = lax.div(me, 4)
    mate = me + 1 - 2 * core
    xnbr = me + 2 - 4 * xpos
    ynbr = me + 4 - 8 * ypos
    diag = xnbr + 4 - 8 * ypos
    depth = wk_in.shape[0]
    width = wk_in.shape[1]
    cols = tok_in.shape[0]
    pieces = 2 + groups
    wire = tok_in.shape[1] // chunks

    def own_slot(first, size):
        rows = pl.ds(pl.multiple_of(z * cols, 16), cols)
        return tok.at[rows, pl.ds(first, size)]

    def load(first, size, i):
        return pltpu.make_async_copy(tok_in.at[:, pl.ds(first, size)], own_slot(first, size), tok_sem.at[i])

    loads = [load(0, wire, 0), load(wire, wire, 1), load(2 * wire, tok_in.shape[1] - 2 * wire, 2)]
    for copy in loads:
        copy.start()

    barrier = pltpu.get_barrier_semaphore()
    for other in (mate, xnbr, ynbr):
        pl.semaphore_signal(barrier, inc=1, device_id={"fsdp": other}, device_id_type=MESH)

    @pl.when(z > 0)
    def _():
        pl.semaphore_signal(barrier, inc=1, device_id={"seq": z - 1}, device_id_type=MESH)

    @pl.when(z < n - 1)
    def _():
        pl.semaphore_signal(barrier, inc=1, device_id={"seq": z + 1}, device_id_type=MESH)

    peers = 5 - jnp.where(z == 0, 1, 0) - jnp.where(z == n - 1, 1, 0)
    pl.semaphore_wait(barrier, peers)

    def w_own(p):
        if p == 0:
            return wk_in
        if p == 1:
            return wv_in
        return wq_in.at[:, pl.ds((p - 2) * width, width)]

    def w_slot(p, f):
        return w.at[p, pl.ds(pl.multiple_of(f * depth, 16), depth), :]

    def w_mark(p, kind, lane):
        if lane == 0:
            return w_recv.at[3 * pieces]
        return w_recv.at[(lane - 1 if kind == 0 else 2) * pieces + p]

    def w_copy(p, kind, lane):
        shard = (me, xnbr, ynbr, diag)[kind]
        src = w_own(p) if kind == 0 else w_slot(p, shard)
        return pltpu.make_async_remote_copy(
            src_ref=src, dst_ref=w_slot(p, shard),
            send_sem=w_send.at[0], recv_sem=w_mark(p, kind, lane),
            device_id={"fsdp": (mate, xnbr, ynbr)[lane]}, device_id_type=MESH,
        )

    def w_wait(p, i):
        slot = w_slot(p, (xnbr, ynbr, diag)[i])
        pltpu.make_async_copy(slot, slot, w_recv.at[i * pieces + p]).wait()

    def w_bulk(count, sem):
        slots = w.at[:, pl.ds(0, count * depth), :]
        pltpu.make_async_copy(slots, slots, sem).wait()

    def t_slot(s, c):
        first = c * wire if isinstance(c, int) else pl.multiple_of(c * wire, wire)
        return tok.at[pl.ds(pl.multiple_of(s * cols, 16), cols), pl.ds(first, wire)]

    def t_pieces(block, c, side):
        if not isinstance(c, int) or c < chunks - 1:
            return [(t_slot(block, c), c)]
        early_at, late_at = (LATE, 0) if side == 0 else (0, cols - LATE)
        lanes = pl.ds(c * wire, wire)
        pieces_of = []
        for at, size, i in ((early_at, cols - LATE, c), (late_at, LATE, chunks)):
            rows = pl.ds(pl.multiple_of(block * cols + at, 16), size)
            pieces_of.append((tok.at[rows, lanes], i))
        return pieces_of

    def t_copies(block, c, side):
        return [
            pltpu.make_async_remote_copy(
                src_ref=ref, dst_ref=ref,
                send_sem=t_send.at[side, block], recv_sem=t_recv.at[block, i],
                device_id={"seq": z + 1 - 2 * side}, device_id_type=MESH,
            )
            for ref, i in t_pieces(block, c, side)
        ]

    def t_arrivals(block, c, side):
        def wait(ref, i):
            return lambda: pltpu.make_async_copy(ref, ref, t_recv.at[block, i]).wait()

        return [wait(ref, i) for ref, i in t_pieces(block, c, side)]

    def own_tokens(c, do):
        @pl.when(z < n - 1)
        def _():
            for copy in t_copies(z, c, 0):
                do(copy)

        @pl.when(z > 0)
        def _():
            for copy in t_copies(z, c, 1):
                do(copy)

    def own_weights(do):
        for p in range(pieces):
            for lane in (1, 2, 0):
                do(w_copy(p, 0, lane))

    def start(copy):
        copy.start()

    def s_copy(block, side):
        return pltpu.make_async_remote_copy(
            src_ref=ss.at[block], dst_ref=ss.at[block],
            send_sem=s_send.at[0], recv_sem=s_recv.at[block],
            device_id={"seq": z + 1 - 2 * side}, device_id_type=MESH,
        )

    def s_wait(block):
        pltpu.make_async_copy(ss.at[block], ss.at[block], s_recv.at[block]).wait()

    def own_sums(do):
        @pl.when(z < n - 1)
        def _():
            do(s_copy(z, 0))

        @pl.when(z > 0)
        def _():
            do(s_copy(z, 1))

    def first_tokens():
        for c in range(2):
            loads[c].wait()
            own_tokens(c, start)

    first_tokens()

    own_weights(start)
    local = []
    for p in range(pieces):
        local.append(pltpu.make_async_copy(w_own(p), w_slot(p, me), local_sem.at[p]))
    local.append(pltpu.make_async_copy(gain_in, gain_ref.at[0], local_sem.at[pieces]))
    local.append(pltpu.make_async_copy(cos_in, cos_ref, local_sem.at[pieces + 1]))
    local.append(pltpu.make_async_copy(sin_in, sin_ref, local_sem.at[pieces + 2]))
    for copy in local:
        copy.start()
    v_s[:, :, HEAD_DIM:] = jnp.ones((kv, v_s.shape[1], HEAD_DIM), jnp.bfloat16)

    loads[2].wait()
    last = t_slot(z, chunks - 1)[...].astype(jnp.float32)
    ss[z] = jnp.sum(last * last, axis=0, keepdims=True)

    def relay(dist, c):
        @pl.when((z >= dist) & (z < n - 1))
        def _():
            for arrival, copy in zip(t_arrivals(z - dist, c, 0), t_copies(z - dist, c, 0)):
                arrival()
                copy.start()

        @pl.when((z + dist < n) & (z > 0))
        def _():
            for arrival, copy in zip(t_arrivals(z + dist, c, 1), t_copies(z + dist, c, 1)):
                arrival()
                copy.start()

    def relay_sums(dist):
        @pl.when((z >= dist) & (z < n - 1))
        def _():
            s_wait(z - dist)
            s_copy(z - dist, 0).start()

        @pl.when((z + dist < n) & (z > 0))
        def _():
            s_wait(z + dist)
            s_copy(z + dist, 1).start()

    def settle(dist, c, piece=0):
        @pl.when((z >= dist) & (z == n - 1))
        def _():
            t_arrivals(z - dist, c, 0)[piece]()

        @pl.when((z + dist < n) & (z == 0))
        def _():
            t_arrivals(z + dist, c, 1)[piece]()

    def token_round(k):
        for dist in range(n - 2, 0, -1):
            c = k - dist + 1
            if c == chunks - 1 and dist == 1:
                own_tokens(c, start)
            if 0 <= c < chunks:
                relay(dist, c)
        if k + 2 < chunks - 1:
            own_tokens(k + 2, start)

    rounds = chunks + n - 3
    early = min(n + 2, rounds)
    for step in range(max(early, pieces)):
        if step < early:
            token_round(step)
        if step == 1:
            own_sums(start)
        if 2 <= step < n:
            relay_sums(step - 1)
        if step < pieces:
            w_wait(step, 0)
            w_copy(step, 1, 0).start()

            @pl.when(core == 1)
            def _():
                w_copy(step, 1, 2).start()

            w_wait(step, 1)
            w_copy(step, 2, 0).start()

            @pl.when(core == 0)
            def _():
                w_copy(step, 2, 1).start()

    for p in range(pieces):
        w_wait(p, 2)
        w_copy(p, 3, 0).start()
    w_bulk(4, w_recv.at[3 * pieces])
    for copy in local:
        copy.wait()

    scale = 1.0 / (12.0 * 50.0)
    peak = 50.0 * math.log2(math.e)

    R = wire

    def rotate_at(rows):
        cosine = cos_ref[rows, :]
        sine = sin_ref[rows, :]
        return lambda x: (x * cosine + pltpu.roll(x, HEAD_DIM // 2, 1) * sine).astype(jnp.bfloat16)

    def tail():
        length = chunks * wire
        first = length - R
        rows = pl.ds(first, R)
        near = (n - 1) * cols
        left = z == 0
        for dist in range(1, n):
            @pl.when(left)
            def _():
                s_wait(z + dist)

            @pl.when(z == n - 1)
            def _():
                s_wait(z - dist)

        for dist in range(1, n - 1):
            for piece in range(2):
                settle(dist, chunks - 1, piece)
        total = ss[0]
        for s in range(1, n):
            total += ss[s]
        inv = lax.rsqrt(total / (n * cols) + 1e-06)
        inv = jnp.broadcast_to(inv, (R, R)).T[:, :1]
        gain = gain_ref[...]
        some = cols - LATE
        spans = ((0, cols, near), (near, LATE, some), (near + some, 0, LATE))

        def normed(span):
            low, high, size = span
            at = pl.ds(pl.multiple_of(jnp.where(left, low, high), 16), size)
            scales = jnp.where(left, gain[:, low : low + size], gain[:, high : high + size])
            floats = tok[at, rows].T.astype(jnp.float32)
            return (floats * inv * scales).astype(jnp.bfloat16), at

        mine, at = normed(spans[0])
        for p in range(pieces):
            part_ref[p] = jnp.dot(mine, w[p, at, :], preferred_element_type=jnp.float32)
        settle(n - 1, chunks - 1, 0)
        mine, at = normed(spans[1])
        for p in range(pieces):
            part_ref[p] += jnp.dot(mine, w[p, at, :], preferred_element_type=jnp.float32)
        settle(n - 1, chunks - 1, 1)
        mine, at = normed(spans[2])
        turn = rotate_at(rows)

        def project(p):
            return part_ref[p] + jnp.dot(mine, w[p, at, :], preferred_element_type=jnp.float32)

        raw = project(0)
        for h in range(kv):
            k_s[h, rows, :] = turn(raw[:, h * HEAD_DIM : (h + 1) * HEAD_DIM])
        raw = project(1)
        for h in range(kv):
            v_s[h, rows, :HEAD_DIM] = raw[:, h * HEAD_DIM : (h + 1) * HEAD_DIM].astype(jnp.bfloat16)
        for g in range(groups):
            raw = project(2 + g)
            for i in range(kv):
                head = g * kv + i
                at_q = (head % groups) * R
                q_s[head // groups, at_q : at_q + R, :] = turn(raw[:, i * HEAD_DIM : (i + 1) * HEAD_DIM])
        row_id = lax.rem(lax.broadcasted_iota(jnp.int32, (groups * R, ROWS), 0), R)
        mask = lax.broadcasted_iota(jnp.int32, (groups * R, ROWS), 1) <= row_id + (ROWS - R)
        for h in range(kv):
            sums = None
            for low in range(0, length, ROWS):
                keys = pl.ds(low, ROWS)
                s = lax.dot_general(
                    q_s[h, : groups * R, :], k_s[h, keys, :], (((1,), (1,)), ((), ())),
                    preferred_element_type=jnp.float32,
                )
                e = jnp.exp2(jnp.tanh(s * scale) * peak)
                if low + ROWS == length:
                    e = jnp.where(mask, e, 0.0)
                e = jnp.dot(e.astype(jnp.bfloat16), v_s[h, keys, :], preferred_element_type=jnp.float32)
                sums = e if sums is None else sums + e
            for g in range(groups):
                head = h * groups + g
                part = sums[g * R : (g + 1) * R, :]
                out_hbm[rows, head * HEAD_DIM : (head + 1) * HEAD_DIM] = (
                    part[:, :HEAD_DIM] / part[:, HEAD_DIM:]
                ).astype(jnp.bfloat16)

    def chunk(first, low, last, base_count, part):
        rows = pl.ds(first, R)
        for dist in range(1, n):
            settle(dist, part)
        raw = tok[:, rows].T
        floats = raw.astype(jnp.float32)
        total = jnp.sum(floats * floats, axis=-1, keepdims=True)
        inv = lax.rsqrt(total / (n * cols) + 1e-06)
        nrm[:R, :] = (floats * inv * gain_ref[...]).astype(jnp.bfloat16)
        normed = nrm[:R, :]
        rotate = rotate_at(rows)

        raw = jnp.dot(normed, w[0], preferred_element_type=jnp.float32)
        for h in range(kv):
            k_s[h, rows, :] = rotate(raw[:, h * HEAD_DIM : (h + 1) * HEAD_DIM])
        raw = jnp.dot(normed, w[1], preferred_element_type=jnp.float32)
        for h in range(kv):
            v_s[h, rows, :HEAD_DIM] = raw[:, h * HEAD_DIM : (h + 1) * HEAD_DIM].astype(jnp.bfloat16)
        for g in range(groups):
            raw = jnp.dot(normed, w[2 + g], preferred_element_type=jnp.float32)
            for i in range(kv):
                head = g * kv + i
                at = (head % groups) * R
                q_s[head // groups, at : at + R, :] = rotate(
                    raw[:, i * HEAD_DIM : (i + 1) * HEAD_DIM]
                )

        def block(h, keys, mask):
            s = lax.dot_general(
                q_s[h, : groups * R, :], k_s[h, keys, :], (((1,), (1,)), ((), ())),
                preferred_element_type=jnp.float32,
            )
            e = jnp.exp2(jnp.tanh(s * scale) * peak)
            if mask is not None:
                e = jnp.where(mask, e, 0.0)
            return jnp.dot(
                e.astype(jnp.bfloat16), v_s[h, keys, :], preferred_element_type=jnp.float32
            )

        row_id = lax.rem(lax.broadcasted_iota(jnp.int32, (groups * R, last), 0), R)
        mask = lax.broadcasted_iota(jnp.int32, (groups * R, last), 1) <= row_id + (last - R)
        top = pl.ds(low, last)
        for h in range(kv):
            acc[h, : groups * R, :] = block(h, top, mask)

        def inner(j, carry):
            keys = pl.ds(pl.multiple_of(j * ROWS, ROWS), ROWS)
            for h in range(kv):
                acc[h, : groups * R, :] += block(h, keys, None)
            return carry

        lax.fori_loop(0, base_count, inner, 0)
        for h in range(kv):
            for g in range(groups):
                sums = acc[h, g * R : (g + 1) * R, :]
                head = h * groups + g
                out_hbm[rows, head * HEAD_DIM : (head + 1) * HEAD_DIM] = (
                    sums[:, :HEAD_DIM] / sums[:, HEAD_DIM:]
                ).astype(jnp.bfloat16)

    def drain_tokens(block, side):
        sent = tok.at[pl.ds(pl.multiple_of(block * cols, 16), cols), :]
        pltpu.make_async_copy(sent, sent, t_send.at[side, block]).wait()

    def drain_weights():
        @pl.when((z == 0) | (z == n - 1))
        def _():
            pltpu.make_async_copy(ss.at[pl.ds(0, 1)], ss.at[pl.ds(0, 1)], s_send.at[0]).wait()

        @pl.when((z > 0) & (z < n - 1))
        def _():
            sent = ss.at[pl.ds(0, n + 1)]
            pltpu.make_async_copy(sent, sent, s_send.at[0]).wait()

        w_bulk(7, w_send.at[0])

    def body(c, carry):
        @pl.when(c == 2)
        def _():
            drain_weights()

            @pl.when(z == 0)
            def _():
                drain_tokens(z, 0)

            @pl.when(z == n - 1)
            def _():
                drain_tokens(z, 1)

        @pl.when(c == 0)
        def _():
            if early < rounds:
                token_round(early)

        @pl.when(c == 1)
        def _():
            for k in range(early + 1, rounds):
                token_round(k)

        low = pl.multiple_of(c * ROWS, ROWS)
        per = ROWS // R
        for i in range(per):
            first = pl.multiple_of(c * ROWS + i * R, R)
            part = c * per + i
            if i < per - 1:
                chunk(first, low, (i + 1) * R, c, part)
            else:
                @pl.when((part < chunks - 1) | ((z > 0) & (z < n - 1)))
                def _():
                    chunk(first, low, (i + 1) * R, c, part)
        return carry

    lax.fori_loop(0, chunks * wire // ROWS, body, 0)

    @pl.when((z == 0) | (z == n - 1))
    def _():
        tail()

    @pl.when((z > 0) & (z < n - 1))
    def _():
        for side in range(2):
            drain_tokens(z, side)
        for dist in range(1, n - 1):
            @pl.when(z >= dist)
            def _():
                drain_tokens(z - dist, 0)

            @pl.when(z + dist < n)
            def _():
                drain_tokens(z + dist, 1)


def fused(n, fsdp, tokens, gain, w_query, w_key, w_value):
    length, cols = tokens.shape
    depth, width = w_key.shape
    kv = width // HEAD_DIM
    groups = w_query.shape[1] // width
    chunks = length // WIRE
    half = HEAD_DIM // 2
    freqs = 10000.0 ** (-2.0 * np.arange(half) / HEAD_DIM)
    angle = np.arange(length)[:, None] * freqs[None, :]
    cosine = np.concatenate([np.cos(angle)] * 2, axis=1).astype(np.float32)
    sine = np.concatenate([-np.sin(angle), np.sin(angle)], axis=1).astype(np.float32)
    hbm = pl.BlockSpec(memory_space=pl.ANY)
    pieces = 2 + groups
    flops = 2 * length * fsdp * depth * width * pieces
    return pl.pallas_call(
        functools.partial(kernel, n, kv, groups, chunks),
        out_shape=pltpu.VMEM((length, w_query.shape[1]), jnp.bfloat16),
        in_specs=[hbm] * 7,
        out_specs=pl.BlockSpec(memory_space=pltpu.VMEM),
        scratch_shapes=[
            pltpu.VMEM((n * cols, length), jnp.bfloat16),
            pltpu.VMEM((pieces, fsdp * depth, width), jnp.bfloat16),
            pltpu.VMEM((WIRE, n * cols), jnp.bfloat16),
            pltpu.VMEM((kv, groups * WIRE, HEAD_DIM), jnp.bfloat16),
            pltpu.VMEM((kv, length, HEAD_DIM), jnp.bfloat16),
            pltpu.VMEM((kv, length, 2 * HEAD_DIM), jnp.bfloat16),
            pltpu.VMEM((kv, groups * WIRE, 2 * HEAD_DIM), jnp.float32),
            pltpu.VMEM((1, n * cols), jnp.float32),
            pltpu.VMEM((length, HEAD_DIM), jnp.float32),
            pltpu.VMEM((length, HEAD_DIM), jnp.float32),
            pltpu.VMEM((pieces, WIRE, width), jnp.float32),
            pltpu.VMEM((n + 1, 1, WIRE), jnp.float32),
            pltpu.SemaphoreType.DMA((3,)),
            pltpu.SemaphoreType.DMA((3 + pieces,)),
            pltpu.SemaphoreType.DMA((2, n)),
            pltpu.SemaphoreType.DMA((n, chunks + 1)),
            pltpu.SemaphoreType.DMA((1,)),
            pltpu.SemaphoreType.DMA((3 * pieces + 1,)),
            pltpu.SemaphoreType.DMA((1,)),
            pltpu.SemaphoreType.DMA((n,)),
        ],
        compiler_params=pltpu.CompilerParams(
            collective_id=0, has_side_effects=True, vmem_limit_bytes=60 * 1024 * 1024
        ),
        cost_estimate=pl.CostEstimate(flops=flops, bytes_accessed=2 * length * cols, transcendentals=0),
    )(tokens.T, gain, jnp.asarray(cosine), jnp.asarray(sine), w_query, w_key, w_value)


def rotate(values, positions):
    half = values.shape[-1] // 2
    index = jnp.arange(half, dtype=jnp.float32)
    freqs = jnp.power(jnp.float32(10000.0), -2.0 * index / values.shape[-1])
    angle = positions[:, None] * freqs[None, :]
    cosine = jnp.cos(angle)[:, None, :]
    sine = jnp.sin(angle)[:, None, :]
    first = values[..., :half]
    second = values[..., half:]
    return jnp.concatenate(
        [first * cosine - second * sine, second * cosine + first * sine], axis=-1
    )


def local(tokens, gain, w_query, w_key, w_value):
    features = gain.shape[0]
    floats = tokens.astype(jnp.float32)
    square_sum = lax.psum(jnp.sum(floats * floats, axis=-1), "seq")
    inv_rms = lax.rsqrt(square_sum / features + 1e-06)[:, None]
    own_cols = tokens.shape[1]
    gain_part = lax.dynamic_slice_in_dim(gain, lax.axis_index("seq") * own_cols, own_cols, 0)
    own_normed = (floats * inv_rms * gain_part[None, :]).astype(jnp.bfloat16)
    normed = lax.all_gather(own_normed, "seq", axis=1, tiled=True)
    length = normed.shape[0]

    def add_one(piece):
        return jnp.dot(normed, piece, preferred_element_type=jnp.float32)

    query_raw = add_one(lax.all_gather(w_query, "fsdp", axis=0, tiled=True))
    key_raw = add_one(lax.all_gather(w_key, "fsdp", axis=0, tiled=True))
    value_raw = add_one(lax.all_gather(w_value, "fsdp", axis=0, tiled=True))
    local_heads = w_query.shape[1] // HEAD_DIM
    local_kv = w_key.shape[1] // HEAD_DIM
    groups = local_heads // local_kv
    positions = jnp.arange(length, dtype=jnp.float32)
    values = value_raw.astype(jnp.bfloat16).reshape(length, local_kv, HEAD_DIM)
    query = rotate(query_raw.reshape(length, local_heads, HEAD_DIM), positions).astype(jnp.bfloat16)
    query = query.reshape(length, local_kv, groups, HEAD_DIM)
    keys = rotate(key_raw.reshape(length, local_kv, HEAD_DIM), positions).astype(jnp.bfloat16)
    scale = 1.0 / jnp.sqrt(jnp.float32(144.0))
    block_rows = 512
    outputs = []
    for first_row in range(0, length, block_rows):
        extent = first_row + block_rows
        query_block = query[first_row:extent]
        scores = (
            jnp.einsum(
                "lgqd,mgd->gqlm", query_block, keys[:extent], preferred_element_type=jnp.float32
            )
            * scale
        )
        capped = 50.0 * jnp.tanh(scores / 50.0)
        causal = jnp.arange(extent)[None, :] <= (first_row + jnp.arange(block_rows))[:, None]
        exponent = jnp.where(causal[None, None], jnp.exp(capped), 0.0)
        weights = (exponent / jnp.sum(exponent, axis=-1, keepdims=True)).astype(jnp.bfloat16)
        context = jnp.einsum(
            "gqlm,mgd->lgqd", weights, values[:extent], preferred_element_type=jnp.float32
        )
        outputs.append(context.reshape(block_rows, local_heads * HEAD_DIM).astype(jnp.bfloat16))
    return jnp.concatenate(outputs, axis=0)


def solution(mesh):
    n, fsdp = mesh.shape["seq"], mesh.shape["fsdp"]
    in_specs = (P("fsdp", "seq"), P(), P("fsdp", "seq"), P("fsdp", "seq"), P("fsdp", "seq"))
    out_specs = P("fsdp", "seq")

    def step(tokens, gain, w_query, w_key, w_value):
        fits = (
            fsdp == 8
            and n == 4
            and tokens.shape[1] % 16 == 0
            and tokens.shape[1] > LATE
            and tokens.shape[0] % ROWS == 0
            and tokens.shape[0] >= 3 * ROWS
            and w_key.shape[0] % 16 == 0
            and w_query.shape[1] % w_key.shape[1] == 0
        )
        if fits:
            return fused(n, fsdp, tokens, gain, w_query, w_key, w_value)
        return local(tokens, gain, w_query, w_key, w_value)

    return jax.shard_map(step, mesh=mesh, in_specs=in_specs, out_specs=out_specs, check_vma=False)
```

```python
import functools
import math

import jax
import jax.numpy as jnp
import numpy as np
from jax import lax
from jax.experimental import pallas as pl
from jax.experimental.pallas import tpu as pltpu
from jax.sharding import PartitionSpec as P

HEAD_DIM = 128
ROWS = 256
WIRE = 128
LATE = 256
AHEAD = (6, 1)
INNER = 2
MESH = pl.DeviceIdType.MESH


def kernel(
    n, kv, groups, chunks,
    tok_in, gain_in, trig_in, wq_in, wk_in, wv_in, out_hbm,
    tok, w, nrm, q_s, k_s, v_s, acc, gain_ref, trig_ref, part_ref, ss,
    tok_sem, local_sem, t_send, t_recv, w_send, w_recv, s_send, s_recv, ready,
):
    z = lax.axis_index("seq")
    me = lax.axis_index("fsdp")
    core = lax.rem(me, 2)
    xpos = lax.rem(lax.div(me, 2), 2)
    ypos = lax.div(me, 4)
    mate = me + 1 - 2 * core
    xnbr = me + 2 - 4 * xpos
    ynbr = me + 4 - 8 * ypos
    diag = xnbr + 4 - 8 * ypos
    depth = wk_in.shape[0]
    width = wk_in.shape[1]
    cols = tok_in.shape[0]
    pieces = 2 + groups
    wire = tok_in.shape[1] // chunks

    def own_slot(first, size):
        rows = pl.ds(pl.multiple_of(z * cols, 16), cols)
        return tok.at[rows, pl.ds(first, size)]

    def load(first, size, i):
        return pltpu.make_async_copy(tok_in.at[:, pl.ds(first, size)], own_slot(first, size), tok_sem.at[i])

    loads = [load(0, wire, 0), load(wire, wire, 1), load(2 * wire, tok_in.shape[1] - 2 * wire, 2)]
    for copy in loads:
        copy.start()

    barrier = pltpu.get_barrier_semaphore()
    half = n // 2
    down = z >= half
    out = z + 1 - 2 * jnp.where(down, 1, 0)
    far = z - 1 + 2 * jnp.where(down, 1, 0)
    outer = (z == 0) | (z == n - 1)
    links = (
        ((z < half - 1) | (z > half), ~outer, {"seq": out}, {"seq": far}),
        (z == half - 1, z == half, {"seq": z + 1}, {"seq": z - 1}),
        (core == 0, core == 1, {"fsdp": mate}, {"fsdp": mate}),
        (xpos == 0, xpos == 1, {"fsdp": xnbr}, {"fsdp": xnbr}),
        (ypos == 0, ypos == 1, {"fsdp": ynbr}, {"fsdp": ynbr}),
    )
    for below, _, child, _ in links:
        @pl.when(below)
        def _():
            pl.semaphore_signal(barrier, inc=1, device_id=child, device_id_type=MESH)

    parents = sum(jnp.where(above, 1, 0) for _, above, _, _ in links)

    @pl.when(parents > 0)
    def _():
        pl.semaphore_wait(barrier, parents)

    for i, (_, above, _, parent) in enumerate(links):
        @pl.when(above)
        def _():
            pl.semaphore_signal(ready.at[i], inc=1, device_id=parent, device_id_type=MESH)

    def await_child(i):
        @pl.when(links[i][0])
        def _():
            pl.semaphore_wait(ready.at[i], 1)

    def w_own(p):
        if p == 0:
            return wk_in
        if p == 1:
            return wv_in
        return wq_in.at[:, pl.ds((p - 2) * width, width)]

    def w_slot(p, f):
        return w.at[p, pl.ds(pl.multiple_of(f * depth, 16), depth), :]

    def w_mark(p, kind, lane):
        if lane == 0:
            return w_recv.at[3 * pieces]
        return w_recv.at[(lane - 1 if kind == 0 else 2) * pieces + p]

    def w_copy(p, kind, lane):
        shard = (me, xnbr, ynbr, diag)[kind]
        src = w_own(p) if kind == 0 else w_slot(p, shard)
        return pltpu.make_async_remote_copy(
            src_ref=src, dst_ref=w_slot(p, shard),
            send_sem=w_send.at[0], recv_sem=w_mark(p, kind, lane),
            device_id={"fsdp": (mate, xnbr, ynbr)[lane]}, device_id_type=MESH,
        )

    def w_wait(p, i):
        slot = w_slot(p, (xnbr, ynbr, diag)[i])
        pltpu.make_async_copy(slot, slot, w_recv.at[i * pieces + p]).wait()

    def w_bulk(count, sem):
        slots = w.at[:, pl.ds(0, count * depth), :]
        pltpu.make_async_copy(slots, slots, sem).wait()

    def t_slot(s, c):
        first = c * wire if isinstance(c, int) else pl.multiple_of(c * wire, wire)
        return tok.at[pl.ds(pl.multiple_of(s * cols, 16), cols), pl.ds(first, wire)]

    def t_pieces(block, c, side):
        if not isinstance(c, int) or c < chunks - 1:
            return [(t_slot(block, c), c)]
        early_at, late_at = (LATE, 0) if side == 0 else (0, cols - LATE)
        lanes = pl.ds(c * wire, wire)
        pieces_of = []
        for at, size, i in ((early_at, cols - LATE, c), (late_at, LATE, chunks)):
            rows = pl.ds(pl.multiple_of(block * cols + at, 16), size)
            pieces_of.append((tok.at[rows, lanes], i))
        return pieces_of

    def t_copies(block, c, side):
        return [
            pltpu.make_async_remote_copy(
                src_ref=ref, dst_ref=ref,
                send_sem=t_send.at[side, block], recv_sem=t_recv.at[block - side, i],
                device_id={"seq": z + 1 - 2 * side}, device_id_type=MESH,
            )
            for ref, i in t_pieces(block, c, side)
        ]

    def t_arrivals(block, c, side):
        def wait(ref, i):
            return lambda: pltpu.make_async_copy(ref, ref, t_recv.at[block - side, i]).wait()

        return [wait(ref, i) for ref, i in t_pieces(block, c, side)]

    def own_weights(do):
        for p in range(pieces):
            for lane in (1, 2, 0):
                do(w_copy(p, 0, lane))

    def start(copy):
        copy.start()

    def s_copy(block, side):
        return pltpu.make_async_remote_copy(
            src_ref=ss.at[block], dst_ref=ss.at[block],
            send_sem=s_send.at[0], recv_sem=s_recv.at[block - side],
            device_id={"seq": z + 1 - 2 * side}, device_id_type=MESH,
        )

    def s_wait(block, side):
        pltpu.make_async_copy(ss.at[block], ss.at[block], s_recv.at[block - side]).wait()

    def own_sums(do):
        @pl.when(z < n - 1)
        def _():
            do(s_copy(z, 0))

        @pl.when(z > 0)
        def _():
            do(s_copy(z, 1))

    def own_side(c, side, when):
        @pl.when(when)
        def _():
            for copy in t_copies(z, c, side):
                copy.start()

    def outward(c, when=True):
        own_side(c, 1, ~outer & ~down & when)
        own_side(c, 0, ~outer & down & when)

    def inward(c):
        own_side(c, 0, ~down)
        own_side(c, 1, down)

    for c in range(AHEAD[0]):
        if c < 3:
            loads[c].wait()
        if c < AHEAD[1]:
            outward(c)
        else:
            outward(c, core == 0)
    for i in (2, 3, 4):
        await_child(i)
    own_weights(start)
    await_child(0)
    await_child(1)
    for c in range(INNER):
        inward(c)
    local = []
    for p in range(pieces):
        local.append(pltpu.make_async_copy(w_own(p), w_slot(p, me), local_sem.at[0]))
    local.append(pltpu.make_async_copy(gain_in, gain_ref.at[0], local_sem.at[1]))
    local.append(pltpu.make_async_copy(trig_in, trig_ref, local_sem.at[2]))
    for copy in local:
        copy.start()
    v_s[:, :, HEAD_DIM:] = jnp.ones((kv, v_s.shape[1], HEAD_DIM), jnp.bfloat16)

    last = t_slot(z, chunks - 1)[...].astype(jnp.float32)
    ss[z] = jnp.sum(last * last, axis=0, keepdims=True)

    def relay(dist, c):
        @pl.when((z >= dist) & (z < n - 1))
        def _():
            for arrival, copy in zip(t_arrivals(z - dist, c, 0), t_copies(z - dist, c, 0)):
                arrival()
                copy.start()

        @pl.when((z + dist < n) & (z > 0))
        def _():
            for arrival, copy in zip(t_arrivals(z + dist, c, 1), t_copies(z + dist, c, 1)):
                arrival()
                copy.start()

    def relay_sums(dist):
        @pl.when((z >= dist) & (z < n - 1))
        def _():
            s_wait(z - dist, 0)
            s_copy(z - dist, 0).start()

        @pl.when((z + dist < n) & (z > 0))
        def _():
            s_wait(z + dist, 1)
            s_copy(z + dist, 1).start()

    def settle(dist, c, piece=0):
        @pl.when((z >= dist) & (z == n - 1))
        def _():
            t_arrivals(z - dist, c, 0)[piece]()

        @pl.when((z + dist < n) & (z == 0))
        def _():
            t_arrivals(z + dist, c, 1)[piece]()

    def token_round(k):
        for dist in range(n - 2, 0, -1):
            c = k - dist + 1
            if c == chunks - 1 and dist == 1:
                outward(c)
                inward(c)
            if 0 <= c < chunks:
                relay(dist, c)
        for side_core in range(2):
            if k + AHEAD[side_core] < chunks - 1:
                outward(k + AHEAD[side_core], core == side_core)
        if k + INNER < chunks - 1:
            inward(k + INNER)

    rounds = chunks + n - 3
    early = min(n + 2, rounds)
    for step in range(max(early, pieces)):
        if step < early:
            token_round(step)
        if step == 1:
            own_sums(start)
        if 2 <= step < n:
            relay_sums(step - 1)
        if step < pieces:
            w_wait(step, 0)
            w_copy(step, 1, 0).start()

            @pl.when(core == 1)
            def _():
                w_copy(step, 1, 2).start()

            w_wait(step, 1)
            w_copy(step, 2, 0).start()

            @pl.when(core == 0)
            def _():
                w_copy(step, 2, 1).start()

    for p in range(pieces):
        w_wait(p, 2)
        w_copy(p, 3, 0).start()
    w_bulk(4, w_recv.at[3 * pieces])
    w_bulk(1, local_sem.at[0])
    for copy in local[pieces:]:
        copy.wait()

    scale = 1.0 / (12.0 * 50.0)
    peak = 50.0 * math.log2(math.e)

    R = wire

    def rotate_at(rows):
        cosine = trig_ref[0, rows, :]
        sine = trig_ref[1, rows, :]
        return lambda x: (x * cosine + pltpu.roll(x, HEAD_DIM // 2, 1) * sine).astype(jnp.bfloat16)

    def tail():
        length = chunks * wire
        first = length - R
        rows = pl.ds(first, R)
        near = (n - 1) * cols
        left = z == 0
        for dist in range(1, n):
            @pl.when(left)
            def _():
                s_wait(z + dist, 1)

            @pl.when(z == n - 1)
            def _():
                s_wait(z - dist, 0)

        for dist in range(1, n - 1):
            for piece in range(2):
                settle(dist, chunks - 1, piece)
        total = ss[0]
        for s in range(1, n):
            total += ss[s]
        inv = lax.rsqrt(total / (n * cols) + 1e-06)
        inv = jnp.broadcast_to(inv, (R, R)).T[:, :1]
        gain = gain_ref[...]
        some = cols - LATE
        spans = ((0, cols, near), (near, LATE, some), (near + some, 0, LATE))

        def normed(span):
            low, high, size = span
            at = pl.ds(pl.multiple_of(jnp.where(left, low, high), 16), size)
            scales = jnp.where(left, gain[:, low : low + size], gain[:, high : high + size])
            floats = tok[at, rows].T.astype(jnp.float32)
            return (floats * inv * scales).astype(jnp.bfloat16), at

        mine, at = normed(spans[0])
        for p in range(pieces):
            part_ref[p] = jnp.dot(mine, w[p, at, :], preferred_element_type=jnp.float32)
        settle(n - 1, chunks - 1, 0)
        mine, at = normed(spans[1])
        for p in range(pieces):
            part_ref[p] += jnp.dot(mine, w[p, at, :], preferred_element_type=jnp.float32)
        settle(n - 1, chunks - 1, 1)
        mine, at = normed(spans[2])
        turn = rotate_at(rows)

        def project(p):
            return part_ref[p] + jnp.dot(mine, w[p, at, :], preferred_element_type=jnp.float32)

        raw = project(0)
        for h in range(kv):
            k_s[h, rows, :] = turn(raw[:, h * HEAD_DIM : (h + 1) * HEAD_DIM])
        raw = project(1)
        for h in range(kv):
            v_s[h, rows, :HEAD_DIM] = raw[:, h * HEAD_DIM : (h + 1) * HEAD_DIM].astype(jnp.bfloat16)
        for g in range(groups):
            raw = project(2 + g)
            for i in range(kv):
                head = g * kv + i
                at_q = (head % groups) * R
                q_s[head // groups, at_q : at_q + R, :] = turn(raw[:, i * HEAD_DIM : (i + 1) * HEAD_DIM])
        row_id = lax.rem(lax.broadcasted_iota(jnp.int32, (groups * R, ROWS), 0), R)
        mask = lax.broadcasted_iota(jnp.int32, (groups * R, ROWS), 1) <= row_id + (ROWS - R)
        for h in range(kv):
            sums = None
            for low in range(0, length, ROWS):
                keys = pl.ds(low, ROWS)
                s = lax.dot_general(
                    q_s[h, : groups * R, :], k_s[h, keys, :], (((1,), (1,)), ((), ())),
                    preferred_element_type=jnp.float32,
                )
                e = jnp.exp2(jnp.tanh(s * scale) * peak)
                if low + ROWS == length:
                    e = jnp.where(mask, e, 0.0)
                e = jnp.dot(e.astype(jnp.bfloat16), v_s[h, keys, :], preferred_element_type=jnp.float32)
                sums = e if sums is None else sums + e
            for g in range(groups):
                head = h * groups + g
                part = sums[g * R : (g + 1) * R, :]
                out_hbm[rows, head * HEAD_DIM : (head + 1) * HEAD_DIM] = (
                    part[:, :HEAD_DIM] / part[:, HEAD_DIM:]
                ).astype(jnp.bfloat16)

    def chunk(first, low, last, base_count, part):
        rows = pl.ds(first, R)
        for dist in range(1, n):
            settle(dist, part)
        raw = tok[:, rows].T
        floats = raw.astype(jnp.float32)
        total = jnp.sum(floats * floats, axis=-1, keepdims=True)
        inv = lax.rsqrt(total / (n * cols) + 1e-06)
        nrm[:R, :] = (floats * inv * gain_ref[...]).astype(jnp.bfloat16)
        normed = nrm[:R, :]
        rotate = rotate_at(rows)

        raw = jnp.dot(normed, w[0], preferred_element_type=jnp.float32)
        for h in range(kv):
            k_s[h, rows, :] = rotate(raw[:, h * HEAD_DIM : (h + 1) * HEAD_DIM])
        raw = jnp.dot(normed, w[1], preferred_element_type=jnp.float32)
        for h in range(kv):
            v_s[h, rows, :HEAD_DIM] = raw[:, h * HEAD_DIM : (h + 1) * HEAD_DIM].astype(jnp.bfloat16)
        for g in range(groups):
            raw = jnp.dot(normed, w[2 + g], preferred_element_type=jnp.float32)
            for i in range(kv):
                head = g * kv + i
                at = (head % groups) * R
                q_s[head // groups, at : at + R, :] = rotate(
                    raw[:, i * HEAD_DIM : (i + 1) * HEAD_DIM]
                )

        def block(h, keys, mask):
            s = lax.dot_general(
                q_s[h, : groups * R, :], k_s[h, keys, :], (((1,), (1,)), ((), ())),
                preferred_element_type=jnp.float32,
            )
            e = jnp.exp2(jnp.tanh(s * scale) * peak)
            if mask is not None:
                e = jnp.where(mask, e, 0.0)
            return jnp.dot(
                e.astype(jnp.bfloat16), v_s[h, keys, :], preferred_element_type=jnp.float32
            )

        row_id = lax.rem(lax.broadcasted_iota(jnp.int32, (groups * R, last), 0), R)
        mask = lax.broadcasted_iota(jnp.int32, (groups * R, last), 1) <= row_id + (last - R)
        top = pl.ds(low, last)
        for h in range(kv):
            acc[h, : groups * R, :] = block(h, top, mask)

        def inner(j, carry):
            keys = pl.ds(pl.multiple_of(j * ROWS, ROWS), ROWS)
            for h in range(kv):
                acc[h, : groups * R, :] += block(h, keys, None)
            return carry

        lax.fori_loop(0, base_count, inner, 0)
        for h in range(kv):
            for g in range(groups):
                sums = acc[h, g * R : (g + 1) * R, :]
                head = h * groups + g
                out_hbm[rows, head * HEAD_DIM : (head + 1) * HEAD_DIM] = (
                    sums[:, :HEAD_DIM] / sums[:, HEAD_DIM:]
                ).astype(jnp.bfloat16)

    def drain_tokens(block, side):
        sent = tok.at[pl.ds(pl.multiple_of(block * cols, 16), cols), :]
        pltpu.make_async_copy(sent, sent, t_send.at[side, block]).wait()

    def drain_weights():
        @pl.when((z == 0) | (z == n - 1))
        def _():
            pltpu.make_async_copy(ss.at[pl.ds(0, 1)], ss.at[pl.ds(0, 1)], s_send.at[0]).wait()

        @pl.when((z > 0) & (z < n - 1))
        def _():
            sent = ss.at[pl.ds(0, n + 1)]
            pltpu.make_async_copy(sent, sent, s_send.at[0]).wait()

        w_bulk(7, w_send.at[0])

    def body(c, carry):
        @pl.when(c == 2)
        def _():
            drain_weights()

            @pl.when(z == 0)
            def _():
                drain_tokens(z, 0)

            @pl.when(z == n - 1)
            def _():
                drain_tokens(z, 1)

        @pl.when(c == 0)
        def _():
            if early < rounds:
                token_round(early)

        @pl.when(c == 1)
        def _():
            for k in range(early + 1, rounds):
                token_round(k)

        low = pl.multiple_of(c * ROWS, ROWS)
        per = ROWS // R
        for i in range(per):
            first = pl.multiple_of(c * ROWS + i * R, R)
            part = c * per + i
            if i < per - 1:
                chunk(first, low, (i + 1) * R, c, part)
            else:
                @pl.when((part < chunks - 1) | ((z > 0) & (z < n - 1)))
                def _():
                    chunk(first, low, (i + 1) * R, c, part)
        return carry

    lax.fori_loop(0, chunks * wire // ROWS, body, 0)

    @pl.when((z == 0) | (z == n - 1))
    def _():
        tail()

    @pl.when((z > 0) & (z < n - 1))
    def _():
        for side in range(2):
            drain_tokens(z, side)
        for dist in range(1, n - 1):
            @pl.when(z >= dist)
            def _():
                drain_tokens(z - dist, 0)

            @pl.when(z + dist < n)
            def _():
                drain_tokens(z + dist, 1)


def fused(n, fsdp, tokens, gain, w_query, w_key, w_value):
    length, cols = tokens.shape
    depth, width = w_key.shape
    kv = width // HEAD_DIM
    groups = w_query.shape[1] // width
    chunks = length // WIRE
    half = HEAD_DIM // 2
    freqs = 10000.0 ** (-2.0 * np.arange(half) / HEAD_DIM)
    angle = np.arange(length)[:, None] * freqs[None, :]
    cosine = np.concatenate([np.cos(angle)] * 2, axis=1).astype(np.float32)
    sine = np.concatenate([-np.sin(angle), np.sin(angle)], axis=1).astype(np.float32)
    hbm = pl.BlockSpec(memory_space=pl.ANY)
    pieces = 2 + groups
    flops = 2 * length * fsdp * depth * width * pieces
    return pl.pallas_call(
        functools.partial(kernel, n, kv, groups, chunks),
        out_shape=pltpu.VMEM((length, w_query.shape[1]), jnp.bfloat16),
        in_specs=[hbm] * 6,
        out_specs=pl.BlockSpec(memory_space=pltpu.VMEM),
        scratch_shapes=[
            pltpu.VMEM((n * cols, length), jnp.bfloat16),
            pltpu.VMEM((pieces, fsdp * depth, width), jnp.bfloat16),
            pltpu.VMEM((WIRE, n * cols), jnp.bfloat16),
            pltpu.VMEM((kv, groups * WIRE, HEAD_DIM), jnp.bfloat16),
            pltpu.VMEM((kv, length, HEAD_DIM), jnp.bfloat16),
            pltpu.VMEM((kv, length, 2 * HEAD_DIM), jnp.bfloat16),
            pltpu.VMEM((kv, groups * WIRE, 2 * HEAD_DIM), jnp.float32),
            pltpu.VMEM((1, n * cols), jnp.float32),
            pltpu.VMEM((2, length, HEAD_DIM), jnp.float32),
            pltpu.VMEM((pieces, WIRE, width), jnp.float32),
            pltpu.VMEM((n + 1, 1, WIRE), jnp.float32),
            pltpu.SemaphoreType.DMA((3,)),
            pltpu.SemaphoreType.DMA((3,)),
            pltpu.SemaphoreType.DMA((2, n)),
            pltpu.SemaphoreType.DMA((n - 1, chunks + 1)),
            pltpu.SemaphoreType.DMA((1,)),
            pltpu.SemaphoreType.DMA((3 * pieces + 1,)),
            pltpu.SemaphoreType.DMA((1,)),
            pltpu.SemaphoreType.DMA((n - 1,)),
            pltpu.SemaphoreType.REGULAR((5,)),
        ],
        compiler_params=pltpu.CompilerParams(
            collective_id=0, has_side_effects=True, vmem_limit_bytes=60 * 1024 * 1024
        ),
        cost_estimate=pl.CostEstimate(flops=flops, bytes_accessed=2 * length * cols, transcendentals=0),
    )(tokens.T, gain, jnp.asarray(np.stack([cosine, sine])), w_query, w_key, w_value)


def rotate(values, positions):
    half = values.shape[-1] // 2
    index = jnp.arange(half, dtype=jnp.float32)
    freqs = jnp.power(jnp.float32(10000.0), -2.0 * index / values.shape[-1])
    angle = positions[:, None] * freqs[None, :]
    cosine = jnp.cos(angle)[:, None, :]
    sine = jnp.sin(angle)[:, None, :]
    first = values[..., :half]
    second = values[..., half:]
    return jnp.concatenate(
        [first * cosine - second * sine, second * cosine + first * sine], axis=-1
    )


def local(tokens, gain, w_query, w_key, w_value):
    features = gain.shape[0]
    floats = tokens.astype(jnp.float32)
    square_sum = lax.psum(jnp.sum(floats * floats, axis=-1), "seq")
    inv_rms = lax.rsqrt(square_sum / features + 1e-06)[:, None]
    own_cols = tokens.shape[1]
    gain_part = lax.dynamic_slice_in_dim(gain, lax.axis_index("seq") * own_cols, own_cols, 0)
    own_normed = (floats * inv_rms * gain_part[None, :]).astype(jnp.bfloat16)
    normed = lax.all_gather(own_normed, "seq", axis=1, tiled=True)
    length = normed.shape[0]

    def add_one(piece):
        return jnp.dot(normed, piece, preferred_element_type=jnp.float32)

    query_raw = add_one(lax.all_gather(w_query, "fsdp", axis=0, tiled=True))
    key_raw = add_one(lax.all_gather(w_key, "fsdp", axis=0, tiled=True))
    value_raw = add_one(lax.all_gather(w_value, "fsdp", axis=0, tiled=True))
    local_heads = w_query.shape[1] // HEAD_DIM
    local_kv = w_key.shape[1] // HEAD_DIM
    groups = local_heads // local_kv
    positions = jnp.arange(length, dtype=jnp.float32)
    values = value_raw.astype(jnp.bfloat16).reshape(length, local_kv, HEAD_DIM)
    query = rotate(query_raw.reshape(length, local_heads, HEAD_DIM), positions).astype(jnp.bfloat16)
    query = query.reshape(length, local_kv, groups, HEAD_DIM)
    keys = rotate(key_raw.reshape(length, local_kv, HEAD_DIM), positions).astype(jnp.bfloat16)
    scale = 1.0 / jnp.sqrt(jnp.float32(144.0))
    block_rows = 512
    outputs = []
    for first_row in range(0, length, block_rows):
        extent = first_row + block_rows
        query_block = query[first_row:extent]
        scores = (
            jnp.einsum(
                "lgqd,mgd->gqlm", query_block, keys[:extent], preferred_element_type=jnp.float32
            )
            * scale
        )
        capped = 50.0 * jnp.tanh(scores / 50.0)
        causal = jnp.arange(extent)[None, :] <= (first_row + jnp.arange(block_rows))[:, None]
        exponent = jnp.where(causal[None, None], jnp.exp(capped), 0.0)
        weights = (exponent / jnp.sum(exponent, axis=-1, keepdims=True)).astype(jnp.bfloat16)
        context = jnp.einsum(
            "gqlm,mgd->lgqd", weights, values[:extent], preferred_element_type=jnp.float32
        )
        outputs.append(context.reshape(block_rows, local_heads * HEAD_DIM).astype(jnp.bfloat16))
    return jnp.concatenate(outputs, axis=0)


def solution(mesh):
    n, fsdp = mesh.shape["seq"], mesh.shape["fsdp"]
    in_specs = (P("fsdp", "seq"), P(), P("fsdp", "seq"), P("fsdp", "seq"), P("fsdp", "seq"))
    out_specs = P("fsdp", "seq")

    def step(tokens, gain, w_query, w_key, w_value):
        fits = (
            fsdp == 8
            and n == 4
            and tokens.shape[1] % 16 == 0
            and tokens.shape[1] > LATE
            and tokens.shape[0] % ROWS == 0
            and tokens.shape[0] >= 3 * ROWS
            and w_key.shape[0] % 16 == 0
            and w_query.shape[1] % w_key.shape[1] == 0
        )
        if fits:
            return fused(n, fsdp, tokens, gain, w_query, w_key, w_value)
        return local(tokens, gain, w_query, w_key, w_value)

    return jax.shard_map(step, mesh=mesh, in_specs=in_specs, out_specs=out_specs, check_vma=False)
```

```python
import functools
import math

import jax
import jax.numpy as jnp
import numpy as np
from jax import lax
from jax.experimental import pallas as pl
from jax.experimental.pallas import tpu as pltpu
from jax.sharding import PartitionSpec as P

HEAD_DIM = 128
ROWS = 256
WIRE = 128
LATE = 256
AHEAD = (6, 1)
INNER = 2
FIRST = 2
MESH = pl.DeviceIdType.MESH


def kernel(
    n, kv, groups, chunks,
    tok_in, gain_in, trig_in, wq_in, wk_in, wv_in, out_ref, q_s, k_s, v_s,
    tok, w, nrm, acc, gain_ref, trig_ref, part_ref, ss,
    tok_sem, local_sem, t_send, t_recv, w_send, w_recv, s_send, s_recv, ready,
):
    z = lax.axis_index("seq")
    me = lax.axis_index("fsdp")
    core = lax.rem(me, 2)
    xpos = lax.rem(lax.div(me, 2), 2)
    ypos = lax.div(me, 4)
    mate = me + 1 - 2 * core
    xnbr = me + 2 - 4 * xpos
    ynbr = me + 4 - 8 * ypos
    diag = xnbr + 4 - 8 * ypos
    depth = wk_in.shape[0]
    width = wk_in.shape[1]
    cols = tok_in.shape[0]
    pieces = 2 + groups
    wire = tok_in.shape[1] // chunks

    def own_slot(first, size):
        rows = pl.ds(pl.multiple_of(z * cols, 16), cols)
        return tok.at[rows, pl.ds(first, size)]

    def load(first, size, i):
        return pltpu.make_async_copy(tok_in.at[:, pl.ds(first, size)], own_slot(first, size), tok_sem.at[i])

    loads = [load(0, wire, 0), load(wire, wire, 1), load(2 * wire, tok_in.shape[1] - 2 * wire, 2)]
    for copy in loads:
        copy.start()

    barrier = pltpu.get_barrier_semaphore()
    half = n // 2
    down = z >= half
    out = z + 1 - 2 * jnp.where(down, 1, 0)
    far = z - 1 + 2 * jnp.where(down, 1, 0)
    outer = (z == 0) | (z == n - 1)
    links = (
        ((z < half - 1) | (z > half), ~outer, {"seq": out}, {"seq": far}),
        (z == half - 1, z == half, {"seq": z + 1}, {"seq": z - 1}),
        (core == 0, core == 1, {"fsdp": mate}, {"fsdp": mate}),
        (xpos == 0, xpos == 1, {"fsdp": xnbr}, {"fsdp": xnbr}),
        (ypos == 0, ypos == 1, {"fsdp": ynbr}, {"fsdp": ynbr}),
    )
    for below, _, child, _ in links:
        @pl.when(below)
        def _():
            pl.semaphore_signal(barrier, inc=1, device_id=child, device_id_type=MESH)

    parents = sum(jnp.where(above, 1, 0) for _, above, _, _ in links)

    @pl.when(parents > 0)
    def _():
        pl.semaphore_wait(barrier, parents)

    for i, (_, above, _, parent) in enumerate(links):
        @pl.when(above)
        def _():
            pl.semaphore_signal(ready.at[i], inc=1, device_id=parent, device_id_type=MESH)

    def await_child(i):
        @pl.when(links[i][0])
        def _():
            pl.semaphore_wait(ready.at[i], 1)

    def w_own(p):
        if p == 0:
            return wk_in
        if p == 1:
            return wv_in
        return wq_in.at[:, pl.ds((p - 2) * width, width)]

    def w_slot(p, f):
        return w.at[p, pl.ds(pl.multiple_of(f * depth, 16), depth), :]

    def w_mark(p, kind, lane):
        if lane == 0:
            return w_recv.at[3 * pieces]
        return w_recv.at[(lane - 1 if kind == 0 else 2) * pieces + p]

    def w_copy(p, kind, lane):
        shard = (me, xnbr, ynbr, diag)[kind]
        src = w_own(p) if kind == 0 else w_slot(p, shard)
        return pltpu.make_async_remote_copy(
            src_ref=src, dst_ref=w_slot(p, shard),
            send_sem=w_send.at[0], recv_sem=w_mark(p, kind, lane),
            device_id={"fsdp": (mate, xnbr, ynbr)[lane]}, device_id_type=MESH,
        )

    def w_wait(p, i):
        slot = w_slot(p, (xnbr, ynbr, diag)[i])
        pltpu.make_async_copy(slot, slot, w_recv.at[i * pieces + p]).wait()

    def w_bulk(count, sem):
        slots = w.at[:, pl.ds(0, count * depth), :]
        pltpu.make_async_copy(slots, slots, sem).wait()

    def t_slot(s, c):
        first = c * wire if isinstance(c, int) else pl.multiple_of(c * wire, wire)
        return tok.at[pl.ds(pl.multiple_of(s * cols, 16), cols), pl.ds(first, wire)]

    def t_pieces(block, c, side):
        if not isinstance(c, int) or c < chunks - 1:
            return [(t_slot(block, c), c)]
        early_at, late_at = (LATE, 0) if side == 0 else (0, cols - LATE)
        lanes = pl.ds(c * wire, wire)
        pieces_of = []
        for at, size, i in ((early_at, cols - LATE, c), (late_at, LATE, chunks)):
            rows = pl.ds(pl.multiple_of(block * cols + at, 16), size)
            pieces_of.append((tok.at[rows, lanes], i))
        return pieces_of

    def t_copies(block, c, side):
        return [
            pltpu.make_async_remote_copy(
                src_ref=ref, dst_ref=ref,
                send_sem=t_send.at[side, block], recv_sem=t_recv.at[block - side, i],
                device_id={"seq": z + 1 - 2 * side}, device_id_type=MESH,
            )
            for ref, i in t_pieces(block, c, side)
        ]

    def t_arrivals(block, c, side):
        def wait(ref, i):
            return lambda: pltpu.make_async_copy(ref, ref, t_recv.at[block - side, i]).wait()

        return [wait(ref, i) for ref, i in t_pieces(block, c, side)]

    def own_weights(do):
        for p in range(pieces):
            for lane in (1, 2, 0):
                do(w_copy(p, 0, lane))

    def start(copy):
        copy.start()

    def s_copy(block, side):
        return pltpu.make_async_remote_copy(
            src_ref=ss.at[block], dst_ref=ss.at[block],
            send_sem=s_send.at[0], recv_sem=s_recv.at[block - side],
            device_id={"seq": z + 1 - 2 * side}, device_id_type=MESH,
        )

    def s_wait(block, side):
        pltpu.make_async_copy(ss.at[block], ss.at[block], s_recv.at[block - side]).wait()

    def own_sums(do):
        @pl.when(z < n - 1)
        def _():
            do(s_copy(z, 0))

        @pl.when(z > 0)
        def _():
            do(s_copy(z, 1))

    def own_side(c, side, when):
        @pl.when(when)
        def _():
            for copy in t_copies(z, c, side):
                copy.start()

    def outward(c, when=True):
        own_side(c, 1, ~outer & ~down & when)
        own_side(c, 0, ~outer & down & when)

    def inward(c, when=True):
        own_side(c, 0, ~down & when)
        own_side(c, 1, down & when)

    for c in range(AHEAD[0]):
        if c < 3:
            loads[c].wait()
        if c < AHEAD[1]:
            outward(c)
        else:
            outward(c, core == 0)
    for i in (2, 3, 4):
        await_child(i)
    own_weights(start)
    await_child(0)
    await_child(1)
    for c in range(INNER):
        inward(c)
    for c in range(INNER, chunks):
        inward(c, outer)
    local = []
    for p in range(pieces):
        local.append(pltpu.make_async_copy(w_own(p), w_slot(p, me), local_sem.at[0]))
    local.append(pltpu.make_async_copy(gain_in, gain_ref.at[0], local_sem.at[1]))
    local.append(pltpu.make_async_copy(trig_in, trig_ref, local_sem.at[2]))
    for copy in local:
        copy.start()
    v_s[:, :, HEAD_DIM:] = jnp.ones((kv, v_s.shape[1], HEAD_DIM), jnp.bfloat16)

    last = t_slot(z, chunks - 1)[...].astype(jnp.float32)
    ss[z] = jnp.sum(last * last, axis=0, keepdims=True)

    def relay(dist, c):
        @pl.when((z >= dist) & (z < n - 1))
        def _():
            for arrival, copy in zip(t_arrivals(z - dist, c, 0), t_copies(z - dist, c, 0)):
                arrival()
                copy.start()

        @pl.when((z + dist < n) & (z > 0))
        def _():
            for arrival, copy in zip(t_arrivals(z + dist, c, 1), t_copies(z + dist, c, 1)):
                arrival()
                copy.start()

    def relay_sums(dist):
        @pl.when((z >= dist) & (z < n - 1))
        def _():
            s_wait(z - dist, 0)
            s_copy(z - dist, 0).start()

        @pl.when((z + dist < n) & (z > 0))
        def _():
            s_wait(z + dist, 1)
            s_copy(z + dist, 1).start()

    def settle(dist, c, piece=0):
        @pl.when((z >= dist) & (z == n - 1))
        def _():
            t_arrivals(z - dist, c, 0)[piece]()

        @pl.when((z + dist < n) & (z == 0))
        def _():
            t_arrivals(z + dist, c, 1)[piece]()

    def token_round(k):
        for dist in range(n - 2, 0, -1):
            c = k - dist + 1
            if c == chunks - 1 and dist == 1:
                outward(c)
            if 0 <= c < chunks:
                relay(dist, c)
        for side_core in range(2):
            if k + AHEAD[side_core] < chunks - 1:
                outward(k + AHEAD[side_core], core == side_core)
        if k + INNER < chunks:
            inward(k + INNER, ~outer)

    rounds = chunks + n - 3
    early = min(n + 2, rounds)
    for step in range(max(early, pieces)):
        if step < early:
            token_round(step)
        if step == 1:
            own_sums(start)
        if 2 <= step < n:
            relay_sums(step - 1)
        if step < pieces:
            w_wait(step, 0)
            w_copy(step, 1, 0).start()

            @pl.when(core == 1)
            def _():
                w_copy(step, 1, 2).start()

            w_wait(step, 1)
            w_copy(step, 2, 0).start()

            @pl.when(core == 0)
            def _():
                w_copy(step, 2, 1).start()

    for p in range(pieces):
        w_wait(p, 2)
        w_copy(p, 3, 0).start()
    w_bulk(4, w_recv.at[3 * pieces])
    w_bulk(1, local_sem.at[0])
    for copy in local[pieces:]:
        copy.wait()

    scale = 1.0 / (12.0 * 50.0)
    peak = 50.0 * math.log2(math.e)

    R = wire

    def rotate_at(rows):
        cosine = trig_ref[0, rows, :]
        sine = trig_ref[1, rows, :]
        return lambda x: (x * cosine + pltpu.roll(x, HEAD_DIM // 2, 1) * sine).astype(jnp.bfloat16)

    def tail():
        length = chunks * wire
        first = length - R
        rows = pl.ds(first, R)
        near = (n - 1) * cols
        left = z == 0
        for dist in range(1, n):
            @pl.when(left)
            def _():
                s_wait(z + dist, 1)

            @pl.when(z == n - 1)
            def _():
                s_wait(z - dist, 0)

        for dist in range(1, n - 1):
            for piece in range(2):
                settle(dist, chunks - 1, piece)
        total = ss[0]
        for s in range(1, n):
            total += ss[s]
        inv = lax.rsqrt(total / (n * cols) + 1e-06)
        inv = jnp.broadcast_to(inv, (R, R)).T[:, :1]
        gain = gain_ref[...]
        some = cols - LATE
        spans = ((0, cols, near), (near, LATE, some), (near + some, 0, LATE))

        def normed(span):
            low, high, size = span
            at = pl.ds(pl.multiple_of(jnp.where(left, low, high), 16), size)
            scales = jnp.where(left, gain[:, low : low + size], gain[:, high : high + size])
            floats = tok[at, rows].T.astype(jnp.float32)
            return (floats * inv * scales).astype(jnp.bfloat16), at

        mine, at = normed(spans[0])
        for p in range(pieces):
            part_ref[p] = jnp.dot(mine, w[p, at, :], preferred_element_type=jnp.float32)
        settle(n - 1, chunks - 1, 0)
        mine, at = normed(spans[1])
        for p in range(pieces):
            part_ref[p] += jnp.dot(mine, w[p, at, :], preferred_element_type=jnp.float32)
        settle(n - 1, chunks - 1, 1)
        mine, at = normed(spans[2])
        turn = rotate_at(rows)

        def project(p):
            return part_ref[p] + jnp.dot(mine, w[p, at, :], preferred_element_type=jnp.float32)

        raw = project(0)
        for h in range(kv):
            k_s[h, rows, :] = turn(raw[:, h * HEAD_DIM : (h + 1) * HEAD_DIM])
        raw = project(1)
        for h in range(kv):
            v_s[h, rows, :HEAD_DIM] = raw[:, h * HEAD_DIM : (h + 1) * HEAD_DIM].astype(jnp.bfloat16)
        for g in range(groups):
            raw = project(2 + g)
            for i in range(kv):
                head = g * kv + i
                at_q = (head % groups) * R
                q_s[head // groups, at_q : at_q + R, :] = turn(raw[:, i * HEAD_DIM : (i + 1) * HEAD_DIM])

    def attend(rows, low, last, base_count):
        def block(h, keys, mask):
            s = lax.dot_general(
                q_s[h, : groups * R, :], k_s[h, keys, :], (((1,), (1,)), ((), ())),
                preferred_element_type=jnp.float32,
            )
            e = jnp.exp2(jnp.tanh(s * scale) * peak)
            if mask is not None:
                e = jnp.where(mask, e, 0.0)
            return jnp.dot(
                e.astype(jnp.bfloat16), v_s[h, keys, :], preferred_element_type=jnp.float32
            )

        row_id = lax.rem(lax.broadcasted_iota(jnp.int32, (groups * R, last), 0), R)
        mask = lax.broadcasted_iota(jnp.int32, (groups * R, last), 1) <= row_id + (last - R)
        top = pl.ds(low, last)
        for h in range(kv):
            acc[h, : groups * R, :] = block(h, top, mask)

        def inner(j, carry):
            keys = pl.ds(pl.multiple_of(j * ROWS, ROWS), ROWS)
            for h in range(kv):
                acc[h, : groups * R, :] += block(h, keys, None)
            return carry

        lax.fori_loop(0, base_count, inner, 0)
        for h in range(kv):
            for g in range(groups):
                sums = acc[h, g * R : (g + 1) * R, :]
                head = h * groups + g
                out_ref[rows, head * HEAD_DIM : (head + 1) * HEAD_DIM] = (
                    sums[:, :HEAD_DIM] / sums[:, HEAD_DIM:]
                ).astype(jnp.bfloat16)

    def chunk(first, low, last, base_count, part):
        rows = pl.ds(first, R)
        for dist in range(1, n):
            settle(dist, part)
        raw = tok[:, rows].T
        floats = raw.astype(jnp.float32)
        total = jnp.sum(floats * floats, axis=-1, keepdims=True)
        inv = lax.rsqrt(total / (n * cols) + 1e-06)
        nrm[:R, :] = (floats * inv * gain_ref[...]).astype(jnp.bfloat16)
        normed = nrm[:R, :]
        rotate = rotate_at(rows)

        raw = jnp.dot(normed, w[0], preferred_element_type=jnp.float32)
        for h in range(kv):
            k_s[h, rows, :] = rotate(raw[:, h * HEAD_DIM : (h + 1) * HEAD_DIM])
        raw = jnp.dot(normed, w[1], preferred_element_type=jnp.float32)
        for h in range(kv):
            v_s[h, rows, :HEAD_DIM] = raw[:, h * HEAD_DIM : (h + 1) * HEAD_DIM].astype(jnp.bfloat16)
        for g in range(groups):
            raw = jnp.dot(normed, w[2 + g], preferred_element_type=jnp.float32)
            for i in range(kv):
                head = g * kv + i
                at = (head % groups) * R
                q_s[head // groups, at : at + R, :] = rotate(
                    raw[:, i * HEAD_DIM : (i + 1) * HEAD_DIM]
                )

        @pl.when(part < chunks - 1)
        def _():
            attend(rows, low, last, base_count)

    def drain_tokens(block, side):
        sent = tok.at[pl.ds(pl.multiple_of(block * cols, 16), cols), :]
        pltpu.make_async_copy(sent, sent, t_send.at[side, block]).wait()

    def drain_weights():
        @pl.when((z == 0) | (z == n - 1))
        def _():
            pltpu.make_async_copy(ss.at[pl.ds(0, 1)], ss.at[pl.ds(0, 1)], s_send.at[0]).wait()

        @pl.when((z > 0) & (z < n - 1))
        def _():
            sent = ss.at[pl.ds(0, n + 1)]
            pltpu.make_async_copy(sent, sent, s_send.at[0]).wait()

        w_bulk(7, w_send.at[0])

    def body(c, carry):
        @pl.when(c == 2)
        def _():
            drain_weights()

            @pl.when(z == 0)
            def _():
                drain_tokens(z, 0)

            @pl.when(z == n - 1)
            def _():
                drain_tokens(z, 1)

        low = pl.multiple_of(c * ROWS, ROWS)
        per = ROWS // R
        for i in range(per):
            first = pl.multiple_of(c * ROWS + i * R, R)
            part = c * per + i
            for k in range(early, rounds):
                before = 0 if k == early else FIRST + k - early - 1
                if before % per == i:
                    @pl.when(c == before // per)
                    def _():
                        token_round(k)

            if i < per - 1:
                chunk(first, low, (i + 1) * R, c, part)
            else:
                @pl.when((part < chunks - 1) | ((z > 0) & (z < n - 1)))
                def _():
                    chunk(first, low, (i + 1) * R, c, part)
        return carry

    lax.fori_loop(0, chunks * wire // ROWS, body, 0)

    @pl.when((z == 0) | (z == n - 1))
    def _():
        tail()

    @pl.when((z > 0) & (z < n - 1))
    def _():
        for side in range(2):
            drain_tokens(z, side)
        for dist in range(1, n - 1):
            @pl.when(z >= dist)
            def _():
                drain_tokens(z - dist, 0)

            @pl.when(z + dist < n)
            def _():
                drain_tokens(z + dist, 1)


def finish(out_ref, q_s, k_s, v_s, out_hbm, last_ref, sems):
    length, width = out_ref.shape
    kv, tall = q_s.shape[:2]
    groups = tall // WIRE
    R = WIRE
    first = length - R
    scale = 1.0 / (12.0 * 50.0)
    peak = 50.0 * math.log2(math.e)
    done = pl.ds(0, first)
    copies = [pltpu.make_async_copy(out_ref.at[done, :], out_hbm.at[done, :], sems.at[0])]
    copies[0].start()
    rows = pl.ds(first, R)
    row_id = lax.rem(lax.broadcasted_iota(jnp.int32, (groups * R, ROWS), 0), R)
    mask = lax.broadcasted_iota(jnp.int32, (groups * R, ROWS), 1) <= row_id + (ROWS - R)
    for h in range(kv):
        sums = None
        for low in range(0, length, ROWS):
            keys = pl.ds(low, ROWS)
            s = lax.dot_general(
                q_s[h, : groups * R, :], k_s[h, keys, :], (((1,), (1,)), ((), ())),
                preferred_element_type=jnp.float32,
            )
            e = jnp.exp2(jnp.tanh(s * scale) * peak)
            if low + ROWS == length:
                e = jnp.where(mask, e, 0.0)
            e = jnp.dot(e.astype(jnp.bfloat16), v_s[h, keys, :], preferred_element_type=jnp.float32)
            sums = e if sums is None else sums + e
        for g in range(groups):
            head = h * groups + g
            part = sums[g * R : (g + 1) * R, :]
            last_ref[:, head * HEAD_DIM : (head + 1) * HEAD_DIM] = (
                part[:, :HEAD_DIM] / part[:, HEAD_DIM:]
            ).astype(jnp.bfloat16)
        lanes = pl.ds(h * groups * HEAD_DIM, groups * HEAD_DIM)
        copies.append(pltpu.make_async_copy(last_ref.at[:, lanes], out_hbm.at[rows, lanes], sems.at[1 + h]))
        copies[-1].start()
    for copy in copies:
        copy.wait()


def fused(n, fsdp, tokens, gain, w_query, w_key, w_value):
    length, cols = tokens.shape
    depth, width = w_key.shape
    kv = width // HEAD_DIM
    groups = w_query.shape[1] // width
    chunks = length // WIRE
    half = HEAD_DIM // 2
    freqs = 10000.0 ** (-2.0 * np.arange(half) / HEAD_DIM)
    angle = np.arange(length)[:, None] * freqs[None, :]
    cosine = np.concatenate([np.cos(angle)] * 2, axis=1).astype(np.float32)
    sine = np.concatenate([-np.sin(angle), np.sin(angle)], axis=1).astype(np.float32)
    hbm = pl.BlockSpec(memory_space=pl.ANY)
    pieces = 2 + groups
    flops = 2 * length * fsdp * depth * width * pieces
    vmem = pl.BlockSpec(memory_space=pltpu.VMEM)
    heads = w_query.shape[1]
    state = pl.pallas_call(
        functools.partial(kernel, n, kv, groups, chunks),
        out_shape=(
            pltpu.VMEM((length, heads), jnp.bfloat16),
            pltpu.VMEM((kv, groups * WIRE, HEAD_DIM), jnp.bfloat16),
            pltpu.VMEM((kv, length, HEAD_DIM), jnp.bfloat16),
            pltpu.VMEM((kv, length, 2 * HEAD_DIM), jnp.bfloat16),
        ),
        in_specs=[hbm] * 6,
        out_specs=[vmem] * 4,
        scratch_shapes=[
            pltpu.VMEM((n * cols, length), jnp.bfloat16),
            pltpu.VMEM((pieces, fsdp * depth, width), jnp.bfloat16),
            pltpu.VMEM((WIRE, n * cols), jnp.bfloat16),
            pltpu.VMEM((kv, groups * WIRE, 2 * HEAD_DIM), jnp.float32),
            pltpu.VMEM((1, n * cols), jnp.float32),
            pltpu.VMEM((2, length, HEAD_DIM), jnp.float32),
            pltpu.VMEM((pieces, WIRE, width), jnp.float32),
            pltpu.VMEM((n + 1, 1, WIRE), jnp.float32),
            pltpu.SemaphoreType.DMA((3,)),
            pltpu.SemaphoreType.DMA((3,)),
            pltpu.SemaphoreType.DMA((2, n)),
            pltpu.SemaphoreType.DMA((n - 1, chunks + 1)),
            pltpu.SemaphoreType.DMA((1,)),
            pltpu.SemaphoreType.DMA((3 * pieces + 1,)),
            pltpu.SemaphoreType.DMA((1,)),
            pltpu.SemaphoreType.DMA((n - 1,)),
            pltpu.SemaphoreType.REGULAR((5,)),
        ],
        compiler_params=pltpu.CompilerParams(
            collective_id=0, has_side_effects=True, vmem_limit_bytes=58 * 1024 * 1024
        ),
        cost_estimate=pl.CostEstimate(flops=flops, bytes_accessed=2 * length * cols, transcendentals=0),
    )(tokens.T, gain, jnp.asarray(np.stack([cosine, sine])), w_query, w_key, w_value)
    return pl.pallas_call(
        finish,
        out_shape=jax.ShapeDtypeStruct((length, heads), jnp.bfloat16),
        in_specs=[vmem] * 4,
        out_specs=hbm,
        scratch_shapes=[pltpu.VMEM((WIRE, heads), jnp.bfloat16), pltpu.SemaphoreType.DMA((1 + kv,))],
        compiler_params=pltpu.CompilerParams(vmem_limit_bytes=16 * 1024 * 1024),
    )(*(pltpu.with_memory_space_constraint(x, pltpu.VMEM) for x in state))


def rotate(values, positions):
    half = values.shape[-1] // 2
    index = jnp.arange(half, dtype=jnp.float32)
    freqs = jnp.power(jnp.float32(10000.0), -2.0 * index / values.shape[-1])
    angle = positions[:, None] * freqs[None, :]
    cosine = jnp.cos(angle)[:, None, :]
    sine = jnp.sin(angle)[:, None, :]
    first = values[..., :half]
    second = values[..., half:]
    return jnp.concatenate(
        [first * cosine - second * sine, second * cosine + first * sine], axis=-1
    )


def local(tokens, gain, w_query, w_key, w_value):
    features = gain.shape[0]
    floats = tokens.astype(jnp.float32)
    square_sum = lax.psum(jnp.sum(floats * floats, axis=-1), "seq")
    inv_rms = lax.rsqrt(square_sum / features + 1e-06)[:, None]
    own_cols = tokens.shape[1]
    gain_part = lax.dynamic_slice_in_dim(gain, lax.axis_index("seq") * own_cols, own_cols, 0)
    own_normed = (floats * inv_rms * gain_part[None, :]).astype(jnp.bfloat16)
    normed = lax.all_gather(own_normed, "seq", axis=1, tiled=True)
    length = normed.shape[0]

    def add_one(piece):
        return jnp.dot(normed, piece, preferred_element_type=jnp.float32)

    query_raw = add_one(lax.all_gather(w_query, "fsdp", axis=0, tiled=True))
    key_raw = add_one(lax.all_gather(w_key, "fsdp", axis=0, tiled=True))
    value_raw = add_one(lax.all_gather(w_value, "fsdp", axis=0, tiled=True))
    local_heads = w_query.shape[1] // HEAD_DIM
    local_kv = w_key.shape[1] // HEAD_DIM
    groups = local_heads // local_kv
    positions = jnp.arange(length, dtype=jnp.float32)
    values = value_raw.astype(jnp.bfloat16).reshape(length, local_kv, HEAD_DIM)
    query = rotate(query_raw.reshape(length, local_heads, HEAD_DIM), positions).astype(jnp.bfloat16)
    query = query.reshape(length, local_kv, groups, HEAD_DIM)
    keys = rotate(key_raw.reshape(length, local_kv, HEAD_DIM), positions).astype(jnp.bfloat16)
    scale = 1.0 / jnp.sqrt(jnp.float32(144.0))
    block_rows = 512
    outputs = []
    for first_row in range(0, length, block_rows):
        extent = first_row + block_rows
        query_block = query[first_row:extent]
        scores = (
            jnp.einsum(
                "lgqd,mgd->gqlm", query_block, keys[:extent], preferred_element_type=jnp.float32
            )
            * scale
        )
        capped = 50.0 * jnp.tanh(scores / 50.0)
        causal = jnp.arange(extent)[None, :] <= (first_row + jnp.arange(block_rows))[:, None]
        exponent = jnp.where(causal[None, None], jnp.exp(capped), 0.0)
        weights = (exponent / jnp.sum(exponent, axis=-1, keepdims=True)).astype(jnp.bfloat16)
        context = jnp.einsum(
            "gqlm,mgd->lgqd", weights, values[:extent], preferred_element_type=jnp.float32
        )
        outputs.append(context.reshape(block_rows, local_heads * HEAD_DIM).astype(jnp.bfloat16))
    return jnp.concatenate(outputs, axis=0)


def solution(mesh):
    n, fsdp = mesh.shape["seq"], mesh.shape["fsdp"]
    in_specs = (P("fsdp", "seq"), P(), P("fsdp", "seq"), P("fsdp", "seq"), P("fsdp", "seq"))
    out_specs = P("fsdp", "seq")

    def step(tokens, gain, w_query, w_key, w_value):
        fits = (
            fsdp == 8
            and n == 4
            and tokens.shape[1] % 16 == 0
            and tokens.shape[1] > LATE
            and tokens.shape[0] % ROWS == 0
            and tokens.shape[0] >= 3 * ROWS
            and w_key.shape[0] % 16 == 0
            and w_query.shape[1] % w_key.shape[1] == 0
        )
        if fits:
            return fused(n, fsdp, tokens, gain, w_query, w_key, w_value)
        return local(tokens, gain, w_query, w_key, w_value)

    return jax.shard_map(step, mesh=mesh, in_specs=in_specs, out_specs=out_specs, check_vma=False)
```

```python
import functools
import math

import jax
import jax.numpy as jnp
import numpy as np
from jax import lax
from jax.experimental import pallas as pl
from jax.experimental.pallas import tpu as pltpu
from jax.sharding import PartitionSpec as P

HEAD_DIM = 128
ROWS = 256
WIRE = 128
LATE = 256
AHEAD = (5, 1)
INNER = 2
FIRST = 2
DIRECT = 1
MESH = pl.DeviceIdType.MESH


def kernel(
    n, kv, groups, chunks,
    tok_in, gain_in, trig_in, wq_in, wk_in, wv_in, out_ref, q_s, k_s, v_s,
    tok, w, nrm, acc, gain_ref, trig_ref, part_ref, ss,
    tok_sem, local_sem, t_send, t_recv, w_send, w_recv, s_send, s_recv, ready,
):
    z = lax.axis_index("seq")
    me = lax.axis_index("fsdp")
    core = lax.rem(me, 2)
    xpos = lax.rem(lax.div(me, 2), 2)
    ypos = lax.div(me, 4)
    mate = me + 1 - 2 * core
    xnbr = me + 2 - 4 * xpos
    ynbr = me + 4 - 8 * ypos
    diag = xnbr + 4 - 8 * ypos
    depth = wk_in.shape[0]
    width = wk_in.shape[1]
    cols = tok_in.shape[0]
    pieces = 2 + groups
    wire = tok_in.shape[1] // chunks

    def own_slot(first, size):
        rows = pl.ds(pl.multiple_of(z * cols, 16), cols)
        return tok.at[rows, pl.ds(first, size)]

    def load(first, size, i):
        return pltpu.make_async_copy(tok_in.at[:, pl.ds(first, size)], own_slot(first, size), tok_sem.at[i])

    loads = [load(0, wire, 0), load(wire, wire, 1), load(2 * wire, tok_in.shape[1] - 2 * wire, 2)]
    for copy in loads:
        copy.start()

    barrier = pltpu.get_barrier_semaphore()
    half = n // 2
    down = z >= half
    out = z + 1 - 2 * jnp.where(down, 1, 0)
    far = z - 1 + 2 * jnp.where(down, 1, 0)
    outer = (z == 0) | (z == n - 1)
    links = (
        ((z < half - 1) | (z > half), ~outer, {"seq": out}, {"seq": far}),
        (z == half - 1, z == half, {"seq": z + 1}, {"seq": z - 1}),
        (core == 0, core == 1, {"fsdp": mate}, {"fsdp": mate}),
        (xpos == 0, xpos == 1, {"fsdp": xnbr}, {"fsdp": xnbr}),
        (ypos == 0, ypos == 1, {"fsdp": ynbr}, {"fsdp": ynbr}),
    )
    for below, _, child, _ in links:
        @pl.when(below)
        def _():
            pl.semaphore_signal(barrier, inc=1, device_id=child, device_id_type=MESH)

    parents = sum(jnp.where(above, 1, 0) for _, above, _, _ in links)

    @pl.when(parents > 0)
    def _():
        pl.semaphore_wait(barrier, parents)

    for i, (_, above, _, parent) in enumerate(links):
        @pl.when(above)
        def _():
            pl.semaphore_signal(ready.at[max(i - 1, 0)], inc=1, device_id=parent, device_id_type=MESH)

    def await_child(i):
        @pl.when(links[i][0])
        def _():
            pl.semaphore_wait(ready.at[max(i - 1, 0)], 1)

    def w_own(p):
        if p == 0:
            return wk_in
        if p == 1:
            return wv_in
        return wq_in.at[:, pl.ds((p - 2) * width, width)]

    def w_slot(p, f):
        return w.at[p, pl.ds(pl.multiple_of(f * depth, 16), depth), :]

    pair = 2 if pieces % 2 == 0 else 1
    sets = pieces // pair

    def w_mark(p, kind, lane):
        if lane == 0:
            return w_recv.at[2 * sets + 1]
        return w_recv.at[(lane - 1) * sets + p // pair if kind == 0 else 2 * sets]

    def w_copy(p, kind, lane):
        shard = (me, xnbr, ynbr, diag)[kind]
        src = w_own(p) if kind == 0 else w_slot(p, shard)
        return pltpu.make_async_remote_copy(
            src_ref=src, dst_ref=w_slot(p, shard),
            send_sem=w_send.at[0], recv_sem=w_mark(p, kind, lane),
            device_id={"fsdp": (mate, xnbr, ynbr)[lane]}, device_id_type=MESH,
        )

    def w_wait(first, count, shard, sem):
        rows = pl.ds(pl.multiple_of(shard * depth, 16), depth)
        slots = w.at[pl.ds(first, count), rows, :]
        pltpu.make_async_copy(slots, slots, sem).wait()

    def w_bulk(count, sem):
        slots = w.at[:, pl.ds(0, count * depth), :]
        pltpu.make_async_copy(slots, slots, sem).wait()

    def t_slot(s, c):
        first = c * wire if isinstance(c, int) else pl.multiple_of(c * wire, wire)
        return tok.at[pl.ds(pl.multiple_of(s * cols, 16), cols), pl.ds(first, wire)]

    def t_pieces(block, c, side):
        if not isinstance(c, int) or c < chunks - 1:
            return [(t_slot(block, c), c)]
        early_at, late_at = (LATE, 0) if side == 0 else (0, cols - LATE)
        lanes = pl.ds(c * wire, wire)
        pieces_of = []
        for at, size, i in ((early_at, cols - LATE, c), (late_at, LATE, chunks)):
            rows = pl.ds(pl.multiple_of(block * cols + at, 16), size)
            pieces_of.append((tok.at[rows, lanes], i))
        return pieces_of

    def t_copies(block, c, side, direct=False, hop=0):
        return [
            pltpu.make_async_remote_copy(
                src_ref=tok_in.at[:, pl.ds(c * wire, wire)] if direct else ref, dst_ref=ref,
                send_sem=t_send.at[2 * hop + side], recv_sem=t_recv.at[block - side, i],
                device_id={"seq": z + 1 - 2 * side}, device_id_type=MESH,
            )
            for ref, i in t_pieces(block, c, side)
        ]

    def t_arrivals(block, c, side):
        def wait(ref, i):
            return lambda: pltpu.make_async_copy(ref, ref, t_recv.at[block - side, i]).wait()

        return [wait(ref, i) for ref, i in t_pieces(block, c, side)]

    def own_weights(do):
        for p in range(pieces):
            for lane in (1, 2, 0):
                do(w_copy(p, 0, lane))

    def start(copy):
        copy.start()

    def s_copy(block, side):
        return pltpu.make_async_remote_copy(
            src_ref=ss.at[block], dst_ref=ss.at[block],
            send_sem=s_send.at[0], recv_sem=s_recv.at[block - side],
            device_id={"seq": z + 1 - 2 * side}, device_id_type=MESH,
        )

    def s_wait(block, side):
        pltpu.make_async_copy(ss.at[block], ss.at[block], s_recv.at[block - side]).wait()

    def own_sums(do):
        @pl.when(z < n - 1)
        def _():
            do(s_copy(z, 0))

        @pl.when(z > 0)
        def _():
            do(s_copy(z, 1))

    def own_side(c, side, when, direct=False):
        @pl.when(when)
        def _():
            for copy in t_copies(z, c, side, direct):
                copy.start()

    def outward(c, when=True, direct=False):
        own_side(c, 1, ~outer & ~down & when, direct)
        own_side(c, 0, ~outer & down & when, direct)

    def inward(c, when=True):
        own_side(c, 0, ~down & when)
        own_side(c, 1, down & when)

    for c in range(AHEAD[0]):
        direct = c < DIRECT
        if not direct:
            for i in range(DIRECT + 1 if c == DIRECT else 0):
                loads[i].wait()
            if DIRECT < c < 3:
                loads[c].wait()
        outward(c, True if c < AHEAD[1] else core == 0, direct)
    for i in (2, 3, 4):
        await_child(i)
    own_weights(start)
    await_child(0)
    await_child(1)
    for c in range(INNER):
        inward(c)
    for c in range(INNER, chunks):
        inward(c, outer)
    local = []
    for p in range(pieces):
        local.append(pltpu.make_async_copy(w_own(p), w_slot(p, me), local_sem.at[0]))
    local.append(pltpu.make_async_copy(gain_in, gain_ref.at[0], local_sem.at[1]))
    local.append(pltpu.make_async_copy(trig_in, trig_ref, local_sem.at[2]))
    for copy in local:
        copy.start()
    v_s[:, :, HEAD_DIM:] = jnp.ones((kv, v_s.shape[1], HEAD_DIM), jnp.bfloat16)

    last = t_slot(z, chunks - 1)[...].astype(jnp.float32)
    ss[z] = jnp.sum(last * last, axis=0, keepdims=True)

    def relay(dist, c):
        @pl.when((z >= dist) & (z < n - 1))
        def _():
            for arrival, copy in zip(t_arrivals(z - dist, c, 0), t_copies(z - dist, c, 0, hop=dist)):
                arrival()
                copy.start()

        @pl.when((z + dist < n) & (z > 0))
        def _():
            for arrival, copy in zip(t_arrivals(z + dist, c, 1), t_copies(z + dist, c, 1, hop=dist)):
                arrival()
                copy.start()

    def relay_sums(dist):
        @pl.when((z >= dist) & (z < n - 1))
        def _():
            s_wait(z - dist, 0)
            s_copy(z - dist, 0).start()

        @pl.when((z + dist < n) & (z > 0))
        def _():
            s_wait(z + dist, 1)
            s_copy(z + dist, 1).start()

    def settle(dist, c, piece=0):
        @pl.when((z >= dist) & (z == n - 1))
        def _():
            t_arrivals(z - dist, c, 0)[piece]()

        @pl.when((z + dist < n) & (z == 0))
        def _():
            t_arrivals(z + dist, c, 1)[piece]()

    def token_round(k):
        for dist in range(n - 2, 0, -1):
            c = k - dist + 1
            if c == chunks - 1 and dist == 1:
                outward(c)
            if 0 <= c < chunks:
                relay(dist, c)
        for side_core in range(2):
            if k + AHEAD[side_core] < chunks - 1:
                outward(k + AHEAD[side_core], core == side_core)
        if k + INNER < chunks:
            inward(k + INNER, ~outer)

    rounds = chunks + n - 3
    early = min(n + 2, rounds)
    for step in range(max(early, pieces)):
        if step < early:
            token_round(step)
        if step == 1:
            own_sums(start)
        if 2 <= step < n:
            relay_sums(step - 1)
        if step < pieces and step % pair == pair - 1:
            group = range(step + 1 - pair, step + 1)
            w_wait(group[0], pair, xnbr, w_recv.at[step // pair])
            for p in group:
                w_copy(p, 1, 0).start()

            @pl.when(core == 1)
            def _():
                for p in group:
                    w_copy(p, 1, 2).start()

            w_wait(group[0], pair, ynbr, w_recv.at[sets + step // pair])
            for p in group:
                w_copy(p, 2, 0).start()

            @pl.when(core == 0)
            def _():
                for p in group:
                    w_copy(p, 2, 1).start()

    w_wait(0, pieces, diag, w_recv.at[2 * sets])
    for p in range(pieces):
        w_copy(p, 3, 0).start()
    w_bulk(4, w_recv.at[2 * sets + 1])
    w_bulk(1, local_sem.at[0])
    for copy in local[pieces:]:
        copy.wait()

    scale = 1.0 / (12.0 * 50.0)
    peak = 50.0 * math.log2(math.e)

    R = wire

    def rotate_at(rows):
        cosine = trig_ref[0, rows, :]
        sine = trig_ref[1, rows, :]
        return lambda x: (x * cosine + pltpu.roll(x, HEAD_DIM // 2, 1) * sine).astype(jnp.bfloat16)

    def tail():
        length = chunks * wire
        first = length - R
        rows = pl.ds(first, R)
        near = (n - 1) * cols
        left = z == 0
        for dist in range(1, n):
            @pl.when(left)
            def _():
                s_wait(z + dist, 1)

            @pl.when(z == n - 1)
            def _():
                s_wait(z - dist, 0)

        for dist in range(1, n - 1):
            for piece in range(2):
                settle(dist, chunks - 1, piece)
        total = ss[0]
        for s in range(1, n):
            total += ss[s]
        inv = lax.rsqrt(total / (n * cols) + 1e-06)
        inv = jnp.broadcast_to(inv, (R, R)).T[:, :1]
        gain = gain_ref[...]
        some = cols - LATE
        spans = ((0, cols, near), (near, LATE, some), (near + some, 0, LATE))

        def normed(span):
            low, high, size = span
            at = pl.ds(pl.multiple_of(jnp.where(left, low, high), 16), size)
            scales = jnp.where(left, gain[:, low : low + size], gain[:, high : high + size])
            floats = tok[at, rows].T.astype(jnp.float32)
            return (floats * inv * scales).astype(jnp.bfloat16), at

        mine, at = normed(spans[0])
        for p in range(pieces):
            part_ref[p] = jnp.dot(mine, w[p, at, :], preferred_element_type=jnp.float32)
        settle(n - 1, chunks - 1, 0)
        mine, at = normed(spans[1])
        for p in range(pieces):
            part_ref[p] += jnp.dot(mine, w[p, at, :], preferred_element_type=jnp.float32)
        settle(n - 1, chunks - 1, 1)
        mine, at = normed(spans[2])
        turn = rotate_at(rows)

        def project(p):
            return part_ref[p] + jnp.dot(mine, w[p, at, :], preferred_element_type=jnp.float32)

        raw = project(0)
        for h in range(kv):
            k_s[h, rows, :] = turn(raw[:, h * HEAD_DIM : (h + 1) * HEAD_DIM])
        raw = project(1)
        for h in range(kv):
            v_s[h, rows, :HEAD_DIM] = raw[:, h * HEAD_DIM : (h + 1) * HEAD_DIM].astype(jnp.bfloat16)
        for g in range(groups):
            raw = project(2 + g)
            for i in range(kv):
                head = g * kv + i
                at_q = (head % groups) * R
                q_s[head // groups, at_q : at_q + R, :] = turn(raw[:, i * HEAD_DIM : (i + 1) * HEAD_DIM])

    def attend(rows, low, last, base_count):
        def block(h, keys, mask):
            s = lax.dot_general(
                q_s[h, : groups * R, :], k_s[h, keys, :], (((1,), (1,)), ((), ())),
                preferred_element_type=jnp.float32,
            )
            e = jnp.exp2(jnp.tanh(s * scale) * peak)
            if mask is not None:
                e = jnp.where(mask, e, 0.0)
            return jnp.dot(
                e.astype(jnp.bfloat16), v_s[h, keys, :], preferred_element_type=jnp.float32
            )

        row_id = lax.rem(lax.broadcasted_iota(jnp.int32, (groups * R, last), 0), R)
        mask = lax.broadcasted_iota(jnp.int32, (groups * R, last), 1) <= row_id + (last - R)
        top = pl.ds(low, last)
        for h in range(kv):
            acc[h, : groups * R, :] = block(h, top, mask)

        def inner(j, carry):
            keys = pl.ds(pl.multiple_of(j * ROWS, ROWS), ROWS)
            for h in range(kv):
                acc[h, : groups * R, :] += block(h, keys, None)
            return carry

        lax.fori_loop(0, base_count, inner, 0)
        for h in range(kv):
            for g in range(groups):
                sums = acc[h, g * R : (g + 1) * R, :]
                head = h * groups + g
                out_ref[rows, head * HEAD_DIM : (head + 1) * HEAD_DIM] = (
                    sums[:, :HEAD_DIM] / sums[:, HEAD_DIM:]
                ).astype(jnp.bfloat16)

    def chunk(first, low, last, base_count, part):
        rows = pl.ds(first, R)
        for dist in range(1, n):
            settle(dist, part)
        raw = tok[:, rows].T
        floats = raw.astype(jnp.float32)
        total = jnp.sum(floats * floats, axis=-1, keepdims=True)
        inv = lax.rsqrt(total / (n * cols) + 1e-06)
        nrm[:R, :] = (floats * inv * gain_ref[...]).astype(jnp.bfloat16)
        normed = nrm[:R, :]
        rotate = rotate_at(rows)

        raw = jnp.dot(normed, w[0], preferred_element_type=jnp.float32)
        for h in range(kv):
            k_s[h, rows, :] = rotate(raw[:, h * HEAD_DIM : (h + 1) * HEAD_DIM])
        raw = jnp.dot(normed, w[1], preferred_element_type=jnp.float32)
        for h in range(kv):
            v_s[h, rows, :HEAD_DIM] = raw[:, h * HEAD_DIM : (h + 1) * HEAD_DIM].astype(jnp.bfloat16)
        for g in range(groups):
            raw = jnp.dot(normed, w[2 + g], preferred_element_type=jnp.float32)
            for i in range(kv):
                head = g * kv + i
                at = (head % groups) * R
                q_s[head // groups, at : at + R, :] = rotate(
                    raw[:, i * HEAD_DIM : (i + 1) * HEAD_DIM]
                )

        @pl.when(part < chunks - 1)
        def _():
            attend(rows, low, last, base_count)

    def drain_tokens(block, side, hop=0):
        sent = tok.at[pl.ds(pl.multiple_of(block * cols, 16), cols), :]
        pltpu.make_async_copy(sent, sent, t_send.at[2 * hop + side]).wait()

    def drain_weights():
        @pl.when((z == 0) | (z == n - 1))
        def _():
            pltpu.make_async_copy(ss.at[pl.ds(0, 1)], ss.at[pl.ds(0, 1)], s_send.at[0]).wait()

        @pl.when((z > 0) & (z < n - 1))
        def _():
            sent = ss.at[pl.ds(0, n + 1)]
            pltpu.make_async_copy(sent, sent, s_send.at[0]).wait()

        w_bulk(7, w_send.at[0])

    def body(c, carry):
        @pl.when(c == 2)
        def _():
            drain_weights()

            @pl.when(z == 0)
            def _():
                drain_tokens(z, 0)

            @pl.when(z == n - 1)
            def _():
                drain_tokens(z, 1)

        low = pl.multiple_of(c * ROWS, ROWS)
        per = ROWS // R
        for i in range(per):
            first = pl.multiple_of(c * ROWS + i * R, R)
            part = c * per + i
            for k in range(early, rounds):
                before = 0 if k == early else FIRST + k - early - 1
                if before % per == i:
                    @pl.when(c == before // per)
                    def _():
                        token_round(k)

            if i < per - 1:
                chunk(first, low, (i + 1) * R, c, part)
            else:
                @pl.when((part < chunks - 1) | ((z > 0) & (z < n - 1)))
                def _():
                    chunk(first, low, (i + 1) * R, c, part)
        return carry

    lax.fori_loop(0, chunks * wire // ROWS, body, 0)

    @pl.when((z == 0) | (z == n - 1))
    def _():
        tail()

    @pl.when((z > 0) & (z < n - 1))
    def _():
        for side in range(2):
            drain_tokens(z, side)
        for dist in range(1, n - 1):
            @pl.when(z >= dist)
            def _():
                drain_tokens(z - dist, 0, dist)

            @pl.when(z + dist < n)
            def _():
                drain_tokens(z + dist, 1, dist)


def finish(out_ref, q_s, k_s, v_s, out_hbm, last_ref, sems):
    length, width = out_ref.shape
    kv, tall = q_s.shape[:2]
    groups = tall // WIRE
    R = WIRE
    first = length - R
    scale = 1.0 / (12.0 * 50.0)
    peak = 50.0 * math.log2(math.e)
    done = pl.ds(0, first)
    copies = [pltpu.make_async_copy(out_ref.at[done, :], out_hbm.at[done, :], sems.at[0])]
    copies[0].start()
    rows = pl.ds(first, R)
    row_id = lax.rem(lax.broadcasted_iota(jnp.int32, (groups * R, ROWS), 0), R)
    mask = lax.broadcasted_iota(jnp.int32, (groups * R, ROWS), 1) <= row_id + (ROWS - R)
    for h in range(kv):
        sums = None
        for low in range(0, length, ROWS):
            keys = pl.ds(low, ROWS)
            s = lax.dot_general(
                q_s[h, : groups * R, :], k_s[h, keys, :], (((1,), (1,)), ((), ())),
                preferred_element_type=jnp.float32,
            )
            e = jnp.exp2(jnp.tanh(s * scale) * peak)
            if low + ROWS == length:
                e = jnp.where(mask, e, 0.0)
            e = jnp.dot(e.astype(jnp.bfloat16), v_s[h, keys, :], preferred_element_type=jnp.float32)
            sums = e if sums is None else sums + e
        for g in range(groups):
            head = h * groups + g
            part = sums[g * R : (g + 1) * R, :]
            last_ref[:, head * HEAD_DIM : (head + 1) * HEAD_DIM] = (
                part[:, :HEAD_DIM] / part[:, HEAD_DIM:]
            ).astype(jnp.bfloat16)
        lanes = pl.ds(h * groups * HEAD_DIM, groups * HEAD_DIM)
        copies.append(pltpu.make_async_copy(last_ref.at[:, lanes], out_hbm.at[rows, lanes], sems.at[1 + h]))
        copies[-1].start()
    for copy in copies:
        copy.wait()


def fused(n, fsdp, tokens, gain, w_query, w_key, w_value):
    length, cols = tokens.shape
    depth, width = w_key.shape
    kv = width // HEAD_DIM
    groups = w_query.shape[1] // width
    chunks = length // WIRE
    half = HEAD_DIM // 2
    freqs = 10000.0 ** (-2.0 * np.arange(half) / HEAD_DIM)
    angle = np.arange(length)[:, None] * freqs[None, :]
    cosine = np.concatenate([np.cos(angle)] * 2, axis=1).astype(np.float32)
    sine = np.concatenate([-np.sin(angle), np.sin(angle)], axis=1).astype(np.float32)
    hbm = pl.BlockSpec(memory_space=pl.ANY)
    pieces = 2 + groups
    flops = 2 * length * fsdp * depth * width * pieces
    vmem = pl.BlockSpec(memory_space=pltpu.VMEM)
    heads = w_query.shape[1]
    state = pl.pallas_call(
        functools.partial(kernel, n, kv, groups, chunks),
        out_shape=(
            pltpu.VMEM((length, heads), jnp.bfloat16),
            pltpu.VMEM((kv, groups * WIRE, HEAD_DIM), jnp.bfloat16),
            pltpu.VMEM((kv, length, HEAD_DIM), jnp.bfloat16),
            pltpu.VMEM((kv, length, 2 * HEAD_DIM), jnp.bfloat16),
        ),
        in_specs=[hbm] * 6,
        out_specs=[vmem] * 4,
        scratch_shapes=[
            pltpu.VMEM((n * cols, length), jnp.bfloat16),
            pltpu.VMEM((pieces, fsdp * depth, width), jnp.bfloat16),
            pltpu.VMEM((WIRE, n * cols), jnp.bfloat16),
            pltpu.VMEM((kv, groups * WIRE, 2 * HEAD_DIM), jnp.float32),
            pltpu.VMEM((1, n * cols), jnp.float32),
            pltpu.VMEM((2, length, HEAD_DIM), jnp.float32),
            pltpu.VMEM((pieces, WIRE, width), jnp.float32),
            pltpu.VMEM((n + 1, 1, WIRE), jnp.float32),
            pltpu.SemaphoreType.DMA((3,)),
            pltpu.SemaphoreType.DMA((3,)),
            pltpu.SemaphoreType.DMA((2 * (n - 1),)),
            pltpu.SemaphoreType.DMA((n - 1, chunks + 1)),
            pltpu.SemaphoreType.DMA((1,)),
            pltpu.SemaphoreType.DMA((2 * (pieces // 2 if pieces % 2 == 0 else pieces) + 2,)),
            pltpu.SemaphoreType.DMA((1,)),
            pltpu.SemaphoreType.DMA((n - 1,)),
            pltpu.SemaphoreType.REGULAR((4,)),
        ],
        compiler_params=pltpu.CompilerParams(
            collective_id=0, has_side_effects=True, vmem_limit_bytes=58 * 1024 * 1024
        ),
        cost_estimate=pl.CostEstimate(flops=flops, bytes_accessed=2 * length * cols, transcendentals=0),
    )(tokens.T, gain, jnp.asarray(np.stack([cosine, sine])), w_query, w_key, w_value)
    return pl.pallas_call(
        finish,
        out_shape=jax.ShapeDtypeStruct((length, heads), jnp.bfloat16),
        in_specs=[vmem] * 4,
        out_specs=hbm,
        scratch_shapes=[pltpu.VMEM((WIRE, heads), jnp.bfloat16), pltpu.SemaphoreType.DMA((1 + kv,))],
        compiler_params=pltpu.CompilerParams(vmem_limit_bytes=16 * 1024 * 1024),
    )(*(pltpu.with_memory_space_constraint(x, pltpu.VMEM) for x in state))


def rotate(values, positions):
    half = values.shape[-1] // 2
    index = jnp.arange(half, dtype=jnp.float32)
    freqs = jnp.power(jnp.float32(10000.0), -2.0 * index / values.shape[-1])
    angle = positions[:, None] * freqs[None, :]
    cosine = jnp.cos(angle)[:, None, :]
    sine = jnp.sin(angle)[:, None, :]
    first = values[..., :half]
    second = values[..., half:]
    return jnp.concatenate(
        [first * cosine - second * sine, second * cosine + first * sine], axis=-1
    )


def local(tokens, gain, w_query, w_key, w_value):
    features = gain.shape[0]
    floats = tokens.astype(jnp.float32)
    square_sum = lax.psum(jnp.sum(floats * floats, axis=-1), "seq")
    inv_rms = lax.rsqrt(square_sum / features + 1e-06)[:, None]
    own_cols = tokens.shape[1]
    gain_part = lax.dynamic_slice_in_dim(gain, lax.axis_index("seq") * own_cols, own_cols, 0)
    own_normed = (floats * inv_rms * gain_part[None, :]).astype(jnp.bfloat16)
    normed = lax.all_gather(own_normed, "seq", axis=1, tiled=True)
    length = normed.shape[0]

    def add_one(piece):
        return jnp.dot(normed, piece, preferred_element_type=jnp.float32)

    query_raw = add_one(lax.all_gather(w_query, "fsdp", axis=0, tiled=True))
    key_raw = add_one(lax.all_gather(w_key, "fsdp", axis=0, tiled=True))
    value_raw = add_one(lax.all_gather(w_value, "fsdp", axis=0, tiled=True))
    local_heads = w_query.shape[1] // HEAD_DIM
    local_kv = w_key.shape[1] // HEAD_DIM
    groups = local_heads // local_kv
    positions = jnp.arange(length, dtype=jnp.float32)
    values = value_raw.astype(jnp.bfloat16).reshape(length, local_kv, HEAD_DIM)
    query = rotate(query_raw.reshape(length, local_heads, HEAD_DIM), positions).astype(jnp.bfloat16)
    query = query.reshape(length, local_kv, groups, HEAD_DIM)
    keys = rotate(key_raw.reshape(length, local_kv, HEAD_DIM), positions).astype(jnp.bfloat16)
    scale = 1.0 / jnp.sqrt(jnp.float32(144.0))
    block_rows = 512
    outputs = []
    for first_row in range(0, length, block_rows):
        extent = first_row + block_rows
        query_block = query[first_row:extent]
        scores = (
            jnp.einsum(
                "lgqd,mgd->gqlm", query_block, keys[:extent], preferred_element_type=jnp.float32
            )
            * scale
        )
        capped = 50.0 * jnp.tanh(scores / 50.0)
        causal = jnp.arange(extent)[None, :] <= (first_row + jnp.arange(block_rows))[:, None]
        exponent = jnp.where(causal[None, None], jnp.exp(capped), 0.0)
        weights = (exponent / jnp.sum(exponent, axis=-1, keepdims=True)).astype(jnp.bfloat16)
        context = jnp.einsum(
            "gqlm,mgd->lgqd", weights, values[:extent], preferred_element_type=jnp.float32
        )
        outputs.append(context.reshape(block_rows, local_heads * HEAD_DIM).astype(jnp.bfloat16))
    return jnp.concatenate(outputs, axis=0)


def solution(mesh):
    n, fsdp = mesh.shape["seq"], mesh.shape["fsdp"]
    in_specs = (P("fsdp", "seq"), P(), P("fsdp", "seq"), P("fsdp", "seq"), P("fsdp", "seq"))
    out_specs = P("fsdp", "seq")

    def step(tokens, gain, w_query, w_key, w_value):
        fits = (
            fsdp == 8
            and n == 4
            and tokens.shape[1] % 16 == 0
            and tokens.shape[1] > LATE
            and tokens.shape[0] % ROWS == 0
            and tokens.shape[0] >= 3 * ROWS
            and w_key.shape[0] % 16 == 0
            and w_query.shape[1] % w_key.shape[1] == 0
        )
        if fits:
            return fused(n, fsdp, tokens, gain, w_query, w_key, w_value)
        return local(tokens, gain, w_query, w_key, w_value)

    return jax.shard_map(step, mesh=mesh, in_specs=in_specs, out_specs=out_specs, check_vma=False)
```

```python
import functools
import math

import jax
import jax.numpy as jnp
import numpy as np
from jax import lax
from jax.experimental import pallas as pl
from jax.experimental.pallas import tpu as pltpu
from jax.sharding import PartitionSpec as P

HEAD_DIM = 128
ROWS = 256
WIRE = 128
LATE = 256
AHEAD = (5, 1)
INNER = 2
FIRST = 2
DIRECT = 1
MESH = pl.DeviceIdType.MESH


def kernel(
    n, kv, groups, chunks,
    tok_in, gain_in, trig_in, wq_in, wk_in, wv_in, out_ref, q_s, k_s, v_s,
    tok, w, nrm, acc, gain_ref, trig_ref, part_ref, ss,
    tok_sem, local_sem, t_send, t_recv, w_send, w_recv, s_send, s_recv, ready,
):
    z = lax.axis_index("seq")
    me = lax.axis_index("fsdp")
    core = lax.rem(me, 2)
    xpos = lax.rem(lax.div(me, 2), 2)
    ypos = lax.div(me, 4)
    mate = me + 1 - 2 * core
    xnbr = me + 2 - 4 * xpos
    ynbr = me + 4 - 8 * ypos
    diag = xnbr + 4 - 8 * ypos
    depth = wk_in.shape[0]
    width = wk_in.shape[1]
    cols = tok_in.shape[0]
    pieces = 2 + groups
    wire = tok_in.shape[1] // chunks

    def own_slot(first, size):
        rows = pl.ds(pl.multiple_of(z * cols, 16), cols)
        return tok.at[rows, pl.ds(first, size)]

    def load(first, size, i):
        return pltpu.make_async_copy(tok_in.at[:, pl.ds(first, size)], own_slot(first, size), tok_sem.at[i])

    loads = [load(0, wire, 0), load(wire, wire, 1), load(2 * wire, tok_in.shape[1] - 2 * wire, 2)]
    for copy in loads:
        copy.start()

    barrier = pltpu.get_barrier_semaphore()
    half = n // 2
    down = z >= half
    out = z + 1 - 2 * jnp.where(down, 1, 0)
    far = z - 1 + 2 * jnp.where(down, 1, 0)
    outer = (z == 0) | (z == n - 1)
    links = (
        ((z < half - 1) | (z > half), ~outer, {"seq": out}, {"seq": far}),
        (z == half - 1, z == half, {"seq": z + 1}, {"seq": z - 1}),
        (core == 0, core == 1, {"fsdp": mate}, {"fsdp": mate}),
        (xpos == 0, xpos == 1, {"fsdp": xnbr}, {"fsdp": xnbr}),
        (ypos == 0, ypos == 1, {"fsdp": ynbr}, {"fsdp": ynbr}),
    )
    for below, _, child, _ in links:
        @pl.when(below)
        def _():
            pl.semaphore_signal(barrier, inc=1, device_id=child, device_id_type=MESH)

    parents = sum(jnp.where(above, 1, 0) for _, above, _, _ in links)

    @pl.when(parents > 0)
    def _():
        pl.semaphore_wait(barrier, parents)

    for i, (_, above, _, parent) in enumerate(links):
        @pl.when(above)
        def _():
            pl.semaphore_signal(ready.at[max(i - 1, 0)], inc=1, device_id=parent, device_id_type=MESH)

    def await_child(i):
        @pl.when(links[i][0])
        def _():
            pl.semaphore_wait(ready.at[max(i - 1, 0)], 1)

    def w_own(p):
        if p == 0:
            return wk_in
        if p == 1:
            return wv_in
        return wq_in.at[:, pl.ds((p - 2) * width, width)]

    def w_slot(p, f):
        return w.at[p, pl.ds(pl.multiple_of(f * depth, 16), depth), :]

    pair = 2 if pieces % 2 == 0 else 1
    sets = pieces // pair

    def w_mark(p, kind, lane):
        if lane == 0:
            return w_recv.at[2 * sets + 1]
        return w_recv.at[(lane - 1) * sets + p // pair if kind == 0 else 2 * sets]

    def w_copy(p, kind, lane):
        shard = (me, xnbr, ynbr, diag)[kind]
        src = w_own(p) if kind == 0 else w_slot(p, shard)
        return pltpu.make_async_remote_copy(
            src_ref=src, dst_ref=w_slot(p, shard),
            send_sem=w_send.at[0], recv_sem=w_mark(p, kind, lane),
            device_id={"fsdp": (mate, xnbr, ynbr)[lane]}, device_id_type=MESH,
        )

    def w_wait(first, count, shard, sem):
        rows = pl.ds(pl.multiple_of(shard * depth, 16), depth)
        slots = w.at[pl.ds(first, count), rows, :]
        pltpu.make_async_copy(slots, slots, sem).wait()

    def w_bulk(count, sem):
        slots = w.at[:, pl.ds(0, count * depth), :]
        pltpu.make_async_copy(slots, slots, sem).wait()

    def t_slot(s, c):
        first = c * wire if isinstance(c, int) else pl.multiple_of(c * wire, wire)
        return tok.at[pl.ds(pl.multiple_of(s * cols, 16), cols), pl.ds(first, wire)]

    def t_pieces(block, c, side):
        if not isinstance(c, int) or c < chunks - 1:
            return [(t_slot(block, c), c)]
        early_at, late_at = (LATE, 0) if side == 0 else (0, cols - LATE)
        lanes = pl.ds(c * wire, wire)
        pieces_of = []
        for at, size, i in ((early_at, cols - LATE, c), (late_at, LATE, chunks)):
            rows = pl.ds(pl.multiple_of(block * cols + at, 16), size)
            pieces_of.append((tok.at[rows, lanes], i))
        return pieces_of

    def t_copies(block, c, side, direct=False, hop=0):
        return [
            pltpu.make_async_remote_copy(
                src_ref=tok_in.at[:, pl.ds(c * wire, wire)] if direct else ref, dst_ref=ref,
                send_sem=t_send.at[2 * hop + side], recv_sem=t_recv.at[block - side, i],
                device_id={"seq": z + 1 - 2 * side}, device_id_type=MESH,
            )
            for ref, i in t_pieces(block, c, side)
        ]

    def t_arrivals(block, c, side):
        def wait(ref, i):
            return lambda: pltpu.make_async_copy(ref, ref, t_recv.at[block - side, i]).wait()

        return [wait(ref, i) for ref, i in t_pieces(block, c, side)]

    def own_weights(do):
        for p in range(pieces):
            for lane in (1, 2, 0):
                do(w_copy(p, 0, lane))

    def start(copy):
        copy.start()

    def s_copy(block, side):
        return pltpu.make_async_remote_copy(
            src_ref=ss.at[block], dst_ref=ss.at[block],
            send_sem=s_send.at[0], recv_sem=s_recv.at[block - side],
            device_id={"seq": z + 1 - 2 * side}, device_id_type=MESH,
        )

    def s_wait(block, side):
        pltpu.make_async_copy(ss.at[block], ss.at[block], s_recv.at[block - side]).wait()

    def own_sums(do):
        @pl.when(z < n - 1)
        def _():
            do(s_copy(z, 0))

        @pl.when(z > 0)
        def _():
            do(s_copy(z, 1))

    def own_side(c, side, when, direct=False):
        @pl.when(when)
        def _():
            for copy in t_copies(z, c, side, direct):
                copy.start()

    def outward(c, when=True, direct=False):
        own_side(c, 1, ~outer & ~down & when, direct)
        own_side(c, 0, ~outer & down & when, direct)

    def inward(c, when=True):
        own_side(c, 0, ~down & when)
        own_side(c, 1, down & when)

    for c in range(AHEAD[0]):
        direct = c < DIRECT
        if not direct:
            for i in range(DIRECT + 1 if c == DIRECT else 0):
                loads[i].wait()
            if DIRECT < c < 3:
                loads[c].wait()
        outward(c, True if c < AHEAD[1] else core == 0, direct)
    for i in (2, 3, 4):
        await_child(i)
    own_weights(start)
    await_child(0)
    await_child(1)
    for c in range(INNER):
        inward(c)
    for c in range(INNER, chunks):
        inward(c, outer)
    local = []
    for p in range(pieces):
        local.append(pltpu.make_async_copy(w_own(p), w_slot(p, me), local_sem.at[0]))
    local.append(pltpu.make_async_copy(gain_in, gain_ref.at[0], local_sem.at[1]))
    local.append(pltpu.make_async_copy(trig_in, trig_ref, local_sem.at[2]))
    for copy in local:
        copy.start()
    v_s[:, :, HEAD_DIM:] = jnp.ones((kv, v_s.shape[1], HEAD_DIM), jnp.bfloat16)

    last = t_slot(z, chunks - 1)[...].astype(jnp.float32)
    ss[z] = jnp.sum(last * last, axis=0, keepdims=True)

    def relay(dist, c):
        @pl.when((z >= dist) & (z < n - 1))
        def _():
            for arrival, copy in zip(t_arrivals(z - dist, c, 0), t_copies(z - dist, c, 0, hop=dist)):
                arrival()
                copy.start()

        @pl.when((z + dist < n) & (z > 0))
        def _():
            for arrival, copy in zip(t_arrivals(z + dist, c, 1), t_copies(z + dist, c, 1, hop=dist)):
                arrival()
                copy.start()

    def relay_sums(dist):
        @pl.when((z >= dist) & (z < n - 1))
        def _():
            s_wait(z - dist, 0)
            s_copy(z - dist, 0).start()

        @pl.when((z + dist < n) & (z > 0))
        def _():
            s_wait(z + dist, 1)
            s_copy(z + dist, 1).start()

    def settle(dist, c, piece=0):
        @pl.when((z >= dist) & (z == n - 1))
        def _():
            t_arrivals(z - dist, c, 0)[piece]()

        @pl.when((z + dist < n) & (z == 0))
        def _():
            t_arrivals(z + dist, c, 1)[piece]()

    def token_round(k):
        for dist in range(n - 2, 0, -1):
            c = k - dist + 1
            if c == chunks - 1 and dist == 1:
                outward(c)
            if 0 <= c < chunks:
                relay(dist, c)
        for side_core in range(2):
            if k + AHEAD[side_core] < chunks - 1:
                outward(k + AHEAD[side_core], core == side_core)
        if k + INNER < chunks:
            inward(k + INNER, ~outer)

    rounds = chunks + n - 3
    early = min(n + 2, rounds)
    for step in range(max(early, pieces)):
        if step < early:
            token_round(step)
        if step == 2:
            own_sums(start)
        if 3 <= step <= n:
            relay_sums(step - 2)
        if step < pieces and step % pair == pair - 1:
            group = range(step + 1 - pair, step + 1)
            w_wait(group[0], pair, xnbr, w_recv.at[step // pair])
            for p in group:
                w_copy(p, 1, 0).start()

            @pl.when(core == 1)
            def _():
                for p in group:
                    w_copy(p, 1, 2).start()

            w_wait(group[0], pair, ynbr, w_recv.at[sets + step // pair])
            for p in group:
                w_copy(p, 2, 0).start()

            @pl.when(core == 0)
            def _():
                for p in group:
                    w_copy(p, 2, 1).start()

    w_wait(0, pieces, diag, w_recv.at[2 * sets])
    for p in range(pieces):
        w_copy(p, 3, 0).start()
    w_bulk(4, w_recv.at[2 * sets + 1])
    w_bulk(1, local_sem.at[0])
    for copy in local[pieces:]:
        copy.wait()

    scale = 1.0 / (12.0 * 50.0)
    peak = 50.0 * math.log2(math.e)

    R = wire

    def rotate_at(rows):
        cosine = trig_ref[0, rows, :]
        sine = trig_ref[1, rows, :]
        return lambda x: (x * cosine + pltpu.roll(x, HEAD_DIM // 2, 1) * sine).astype(jnp.bfloat16)

    def tail():
        length = chunks * wire
        first = length - R
        rows = pl.ds(first, R)
        near = (n - 1) * cols
        left = z == 0
        for dist in range(1, n):
            @pl.when(left)
            def _():
                s_wait(z + dist, 1)

            @pl.when(z == n - 1)
            def _():
                s_wait(z - dist, 0)

        for dist in range(1, n - 1):
            for piece in range(2):
                settle(dist, chunks - 1, piece)
        total = ss[0]
        for s in range(1, n):
            total += ss[s]
        inv = lax.rsqrt(total / (n * cols) + 1e-06)
        inv = jnp.broadcast_to(inv, (R, R)).T[:, :1]
        gain = gain_ref[...]
        some = cols - LATE
        spans = ((0, cols, near), (near, LATE, some), (near + some, 0, LATE))

        def normed(span):
            low, high, size = span
            at = pl.ds(pl.multiple_of(jnp.where(left, low, high), 16), size)
            scales = jnp.where(left, gain[:, low : low + size], gain[:, high : high + size])
            floats = tok[at, rows].T.astype(jnp.float32)
            return (floats * inv * scales).astype(jnp.bfloat16), at

        mine, at = normed(spans[0])
        for p in range(pieces):
            part_ref[p] = jnp.dot(mine, w[p, at, :], preferred_element_type=jnp.float32)
        settle(n - 1, chunks - 1, 0)
        mine, at = normed(spans[1])
        for p in range(pieces):
            part_ref[p] += jnp.dot(mine, w[p, at, :], preferred_element_type=jnp.float32)
        settle(n - 1, chunks - 1, 1)
        mine, at = normed(spans[2])
        turn = rotate_at(rows)

        def project(p):
            return part_ref[p] + jnp.dot(mine, w[p, at, :], preferred_element_type=jnp.float32)

        raw = project(0)
        for h in range(kv):
            k_s[h, rows, :] = turn(raw[:, h * HEAD_DIM : (h + 1) * HEAD_DIM])
        raw = project(1)
        for h in range(kv):
            v_s[h, rows, :HEAD_DIM] = raw[:, h * HEAD_DIM : (h + 1) * HEAD_DIM].astype(jnp.bfloat16)
        for g in range(groups):
            raw = project(2 + g)
            for i in range(kv):
                head = g * kv + i
                at_q = (head % groups) * R
                q_s[head // groups, at_q : at_q + R, :] = turn(raw[:, i * HEAD_DIM : (i + 1) * HEAD_DIM])

    def attend(rows, low, last, base_count):
        def block(h, keys, mask):
            s = lax.dot_general(
                q_s[h, : groups * R, :], k_s[h, keys, :], (((1,), (1,)), ((), ())),
                preferred_element_type=jnp.float32,
            )
            e = jnp.exp2(jnp.tanh(s * scale) * peak)
            if mask is not None:
                e = jnp.where(mask, e, 0.0)
            return jnp.dot(
                e.astype(jnp.bfloat16), v_s[h, keys, :], preferred_element_type=jnp.float32
            )

        row_id = lax.rem(lax.broadcasted_iota(jnp.int32, (groups * R, last), 0), R)
        mask = lax.broadcasted_iota(jnp.int32, (groups * R, last), 1) <= row_id + (last - R)
        top = pl.ds(low, last)
        for h in range(kv):
            acc[h, : groups * R, :] = block(h, top, mask)

        def inner(j, carry):
            keys = pl.ds(pl.multiple_of(j * ROWS, ROWS), ROWS)
            for h in range(kv):
                acc[h, : groups * R, :] += block(h, keys, None)
            return carry

        lax.fori_loop(0, base_count, inner, 0)
        for h in range(kv):
            for g in range(groups):
                sums = acc[h, g * R : (g + 1) * R, :]
                head = h * groups + g
                out_ref[rows, head * HEAD_DIM : (head + 1) * HEAD_DIM] = (
                    sums[:, :HEAD_DIM] / sums[:, HEAD_DIM:]
                ).astype(jnp.bfloat16)

    def chunk(first, low, last, base_count, part):
        rows = pl.ds(first, R)
        for dist in range(1, n):
            settle(dist, part)
        raw = tok[:, rows].T
        floats = raw.astype(jnp.float32)
        total = jnp.sum(floats * floats, axis=-1, keepdims=True)
        inv = lax.rsqrt(total / (n * cols) + 1e-06)
        nrm[:R, :] = (floats * inv * gain_ref[...]).astype(jnp.bfloat16)
        normed = nrm[:R, :]
        rotate = rotate_at(rows)

        raw = jnp.dot(normed, w[0], preferred_element_type=jnp.float32)
        for h in range(kv):
            k_s[h, rows, :] = rotate(raw[:, h * HEAD_DIM : (h + 1) * HEAD_DIM])
        raw = jnp.dot(normed, w[1], preferred_element_type=jnp.float32)
        for h in range(kv):
            v_s[h, rows, :HEAD_DIM] = raw[:, h * HEAD_DIM : (h + 1) * HEAD_DIM].astype(jnp.bfloat16)
        for g in range(groups):
            raw = jnp.dot(normed, w[2 + g], preferred_element_type=jnp.float32)
            for i in range(kv):
                head = g * kv + i
                at = (head % groups) * R
                q_s[head // groups, at : at + R, :] = rotate(
                    raw[:, i * HEAD_DIM : (i + 1) * HEAD_DIM]
                )

        @pl.when(part < chunks - 1)
        def _():
            attend(rows, low, last, base_count)

    def drain_tokens(block, side, hop=0):
        sent = tok.at[pl.ds(pl.multiple_of(block * cols, 16), cols), :]
        pltpu.make_async_copy(sent, sent, t_send.at[2 * hop + side]).wait()

    def drain_weights():
        @pl.when((z == 0) | (z == n - 1))
        def _():
            pltpu.make_async_copy(ss.at[pl.ds(0, 1)], ss.at[pl.ds(0, 1)], s_send.at[0]).wait()

        @pl.when((z > 0) & (z < n - 1))
        def _():
            sent = ss.at[pl.ds(0, n + 1)]
            pltpu.make_async_copy(sent, sent, s_send.at[0]).wait()

        w_bulk(7, w_send.at[0])

    def body(c, carry):
        @pl.when(c == 2)
        def _():
            drain_weights()

            @pl.when(z == 0)
            def _():
                drain_tokens(z, 0)

            @pl.when(z == n - 1)
            def _():
                drain_tokens(z, 1)

        low = pl.multiple_of(c * ROWS, ROWS)
        per = ROWS // R
        for i in range(per):
            first = pl.multiple_of(c * ROWS + i * R, R)
            part = c * per + i
            for k in range(early, rounds):
                before = 0 if k == early else FIRST + k - early - 1
                if before % per == i:
                    @pl.when(c == before // per)
                    def _():
                        token_round(k)

            if i < per - 1:
                chunk(first, low, (i + 1) * R, c, part)
            else:
                @pl.when((part < chunks - 1) | ((z > 0) & (z < n - 1)))
                def _():
                    chunk(first, low, (i + 1) * R, c, part)
        return carry

    lax.fori_loop(0, chunks * wire // ROWS, body, 0)

    @pl.when((z == 0) | (z == n - 1))
    def _():
        tail()

    @pl.when((z > 0) & (z < n - 1))
    def _():
        for side in range(2):
            drain_tokens(z, side)
        for dist in range(1, n - 1):
            @pl.when(z >= dist)
            def _():
                drain_tokens(z - dist, 0, dist)

            @pl.when(z + dist < n)
            def _():
                drain_tokens(z + dist, 1, dist)


def finish(out_ref, q_s, k_s, v_s, out_hbm, last_ref, sems):
    length, width = out_ref.shape
    kv, tall = q_s.shape[:2]
    groups = tall // WIRE
    R = WIRE
    first = length - R
    scale = 1.0 / (12.0 * 50.0)
    peak = 50.0 * math.log2(math.e)
    done = pl.ds(0, first)
    copies = [pltpu.make_async_copy(out_ref.at[done, :], out_hbm.at[done, :], sems.at[0])]
    copies[0].start()
    rows = pl.ds(first, R)
    row_id = lax.rem(lax.broadcasted_iota(jnp.int32, (groups * R, ROWS), 0), R)
    mask = lax.broadcasted_iota(jnp.int32, (groups * R, ROWS), 1) <= row_id + (ROWS - R)
    for h in range(kv):
        sums = None
        for low in range(length - ROWS, -1, -ROWS):
            keys = pl.ds(low, ROWS)
            s = lax.dot_general(
                q_s[h, : groups * R, :], k_s[h, keys, :], (((1,), (1,)), ((), ())),
                preferred_element_type=jnp.float32,
            )
            e = jnp.exp2(jnp.tanh(s * scale) * peak)
            if low + ROWS == length:
                e = jnp.where(mask, e, 0.0)
            e = jnp.dot(e.astype(jnp.bfloat16), v_s[h, keys, :], preferred_element_type=jnp.float32)
            sums = e if sums is None else sums + e
        for g in range(groups):
            head = h * groups + g
            part = sums[g * R : (g + 1) * R, :]
            last_ref[:, head * HEAD_DIM : (head + 1) * HEAD_DIM] = (
                part[:, :HEAD_DIM] / part[:, HEAD_DIM:]
            ).astype(jnp.bfloat16)
        lanes = pl.ds(h * groups * HEAD_DIM, groups * HEAD_DIM)
        copies.append(pltpu.make_async_copy(last_ref.at[:, lanes], out_hbm.at[rows, lanes], sems.at[1 + h]))
        copies[-1].start()
    for copy in copies:
        copy.wait()


def fused(n, fsdp, tokens, gain, w_query, w_key, w_value):
    length, cols = tokens.shape
    depth, width = w_key.shape
    kv = width // HEAD_DIM
    groups = w_query.shape[1] // width
    chunks = length // WIRE
    half = HEAD_DIM // 2
    freqs = 10000.0 ** (-2.0 * np.arange(half) / HEAD_DIM)
    angle = np.arange(length)[:, None] * freqs[None, :]
    cosine = np.concatenate([np.cos(angle)] * 2, axis=1).astype(np.float32)
    sine = np.concatenate([-np.sin(angle), np.sin(angle)], axis=1).astype(np.float32)
    hbm = pl.BlockSpec(memory_space=pl.ANY)
    pieces = 2 + groups
    flops = 2 * length * fsdp * depth * width * pieces
    vmem = pl.BlockSpec(memory_space=pltpu.VMEM)
    heads = w_query.shape[1]
    state = pl.pallas_call(
        functools.partial(kernel, n, kv, groups, chunks),
        out_shape=(
            pltpu.VMEM((length, heads), jnp.bfloat16),
            pltpu.VMEM((kv, groups * WIRE, HEAD_DIM), jnp.bfloat16),
            pltpu.VMEM((kv, length, HEAD_DIM), jnp.bfloat16),
            pltpu.VMEM((kv, length, 2 * HEAD_DIM), jnp.bfloat16),
        ),
        in_specs=[hbm] * 6,
        out_specs=[vmem] * 4,
        scratch_shapes=[
            pltpu.VMEM((n * cols, length), jnp.bfloat16),
            pltpu.VMEM((pieces, fsdp * depth, width), jnp.bfloat16),
            pltpu.VMEM((WIRE, n * cols), jnp.bfloat16),
            pltpu.VMEM((kv, groups * WIRE, 2 * HEAD_DIM), jnp.float32),
            pltpu.VMEM((1, n * cols), jnp.float32),
            pltpu.VMEM((2, length, HEAD_DIM), jnp.float32),
            pltpu.VMEM((pieces, WIRE, width), jnp.float32),
            pltpu.VMEM((n + 1, 1, WIRE), jnp.float32),
            pltpu.SemaphoreType.DMA((3,)),
            pltpu.SemaphoreType.DMA((3,)),
            pltpu.SemaphoreType.DMA((2 * (n - 1),)),
            pltpu.SemaphoreType.DMA((n - 1, chunks + 1)),
            pltpu.SemaphoreType.DMA((1,)),
            pltpu.SemaphoreType.DMA((2 * (pieces // 2 if pieces % 2 == 0 else pieces) + 2,)),
            pltpu.SemaphoreType.DMA((1,)),
            pltpu.SemaphoreType.DMA((n - 1,)),
            pltpu.SemaphoreType.REGULAR((4,)),
        ],
        compiler_params=pltpu.CompilerParams(
            collective_id=0, has_side_effects=True, vmem_limit_bytes=58 * 1024 * 1024
        ),
        cost_estimate=pl.CostEstimate(flops=flops, bytes_accessed=2 * length * cols, transcendentals=0),
    )(tokens.T, gain, jnp.asarray(np.stack([cosine, sine])), w_query, w_key, w_value)
    return pl.pallas_call(
        finish,
        out_shape=jax.ShapeDtypeStruct((length, heads), jnp.bfloat16),
        in_specs=[vmem] * 4,
        out_specs=hbm,
        scratch_shapes=[pltpu.VMEM((WIRE, heads), jnp.bfloat16), pltpu.SemaphoreType.DMA((1 + kv,))],
        compiler_params=pltpu.CompilerParams(vmem_limit_bytes=16 * 1024 * 1024),
    )(*(pltpu.with_memory_space_constraint(x, pltpu.VMEM) for x in state))


def rotate(values, positions):
    half = values.shape[-1] // 2
    index = jnp.arange(half, dtype=jnp.float32)
    freqs = jnp.power(jnp.float32(10000.0), -2.0 * index / values.shape[-1])
    angle = positions[:, None] * freqs[None, :]
    cosine = jnp.cos(angle)[:, None, :]
    sine = jnp.sin(angle)[:, None, :]
    first = values[..., :half]
    second = values[..., half:]
    return jnp.concatenate(
        [first * cosine - second * sine, second * cosine + first * sine], axis=-1
    )


def local(tokens, gain, w_query, w_key, w_value):
    features = gain.shape[0]
    floats = tokens.astype(jnp.float32)
    square_sum = lax.psum(jnp.sum(floats * floats, axis=-1), "seq")
    inv_rms = lax.rsqrt(square_sum / features + 1e-06)[:, None]
    own_cols = tokens.shape[1]
    gain_part = lax.dynamic_slice_in_dim(gain, lax.axis_index("seq") * own_cols, own_cols, 0)
    own_normed = (floats * inv_rms * gain_part[None, :]).astype(jnp.bfloat16)
    normed = lax.all_gather(own_normed, "seq", axis=1, tiled=True)
    length = normed.shape[0]

    def add_one(piece):
        return jnp.dot(normed, piece, preferred_element_type=jnp.float32)

    query_raw = add_one(lax.all_gather(w_query, "fsdp", axis=0, tiled=True))
    key_raw = add_one(lax.all_gather(w_key, "fsdp", axis=0, tiled=True))
    value_raw = add_one(lax.all_gather(w_value, "fsdp", axis=0, tiled=True))
    local_heads = w_query.shape[1] // HEAD_DIM
    local_kv = w_key.shape[1] // HEAD_DIM
    groups = local_heads // local_kv
    positions = jnp.arange(length, dtype=jnp.float32)
    values = value_raw.astype(jnp.bfloat16).reshape(length, local_kv, HEAD_DIM)
    query = rotate(query_raw.reshape(length, local_heads, HEAD_DIM), positions).astype(jnp.bfloat16)
    query = query.reshape(length, local_kv, groups, HEAD_DIM)
    keys = rotate(key_raw.reshape(length, local_kv, HEAD_DIM), positions).astype(jnp.bfloat16)
    scale = 1.0 / jnp.sqrt(jnp.float32(144.0))
    block_rows = 512
    outputs = []
    for first_row in range(0, length, block_rows):
        extent = first_row + block_rows
        query_block = query[first_row:extent]
        scores = (
            jnp.einsum(
                "lgqd,mgd->gqlm", query_block, keys[:extent], preferred_element_type=jnp.float32
            )
            * scale
        )
        capped = 50.0 * jnp.tanh(scores / 50.0)
        causal = jnp.arange(extent)[None, :] <= (first_row + jnp.arange(block_rows))[:, None]
        exponent = jnp.where(causal[None, None], jnp.exp(capped), 0.0)
        weights = (exponent / jnp.sum(exponent, axis=-1, keepdims=True)).astype(jnp.bfloat16)
        context = jnp.einsum(
            "gqlm,mgd->lgqd", weights, values[:extent], preferred_element_type=jnp.float32
        )
        outputs.append(context.reshape(block_rows, local_heads * HEAD_DIM).astype(jnp.bfloat16))
    return jnp.concatenate(outputs, axis=0)


def solution(mesh):
    n, fsdp = mesh.shape["seq"], mesh.shape["fsdp"]
    in_specs = (P("fsdp", "seq"), P(), P("fsdp", "seq"), P("fsdp", "seq"), P("fsdp", "seq"))
    out_specs = P("fsdp", "seq")

    def step(tokens, gain, w_query, w_key, w_value):
        fits = (
            fsdp == 8
            and n == 4
            and tokens.shape[1] % 16 == 0
            and tokens.shape[1] > LATE
            and tokens.shape[0] % ROWS == 0
            and tokens.shape[0] >= 3 * ROWS
            and w_key.shape[0] % 16 == 0
            and w_query.shape[1] % w_key.shape[1] == 0
        )
        if fits:
            return fused(n, fsdp, tokens, gain, w_query, w_key, w_value)
        return local(tokens, gain, w_query, w_key, w_value)

    return jax.shard_map(step, mesh=mesh, in_specs=in_specs, out_specs=out_specs, check_vma=False)
```

```python
import functools
import math

import jax
import jax.numpy as jnp
import numpy as np
from jax import lax
from jax.experimental import pallas as pl
from jax.experimental.pallas import tpu as pltpu
from jax.sharding import PartitionSpec as P

HEAD_DIM = 128
ROWS = 256
WIRE = 128
LATE = 256
AHEAD = (5, 1)
INNER = 2
FIRST = 2
DIRECT = 1
MESH = pl.DeviceIdType.MESH


def kernel(
    n, kv, groups, chunks,
    tok_in, gain_in, trig_in, wq_in, wk_in, wv_in, out_ref, q_s, k_s, v_s,
    tok, w, nrm, acc, gain_ref, trig_ref, part_ref, ss,
    tok_sem, local_sem, t_send, t_recv, w_send, w_recv, s_send, s_recv, ready,
):
    z = lax.axis_index("seq")
    me = lax.axis_index("fsdp")
    core = lax.rem(me, 2)
    xpos = lax.rem(lax.div(me, 2), 2)
    ypos = lax.div(me, 4)
    mate = me + 1 - 2 * core
    xnbr = me + 2 - 4 * xpos
    ynbr = me + 4 - 8 * ypos
    diag = xnbr + 4 - 8 * ypos
    depth = wk_in.shape[0]
    width = wk_in.shape[1]
    cols = tok_in.shape[0]
    pieces = 2 + groups
    wire = tok_in.shape[1] // chunks

    def own_slot(first, size):
        rows = pl.ds(pl.multiple_of(z * cols, 16), cols)
        return tok.at[rows, pl.ds(first, size)]

    def load(first, size, i):
        return pltpu.make_async_copy(tok_in.at[:, pl.ds(first, size)], own_slot(first, size), tok_sem.at[i])

    loads = [load(0, wire, 0), load(wire, wire, 1), load(2 * wire, tok_in.shape[1] - 2 * wire, 2)]
    for copy in loads:
        copy.start()

    barrier = pltpu.get_barrier_semaphore()
    half = n // 2
    down = z >= half
    out = z + 1 - 2 * jnp.where(down, 1, 0)
    far = z - 1 + 2 * jnp.where(down, 1, 0)
    outer = (z == 0) | (z == n - 1)
    links = (
        ((z < half - 1) | (z > half), ~outer, {"seq": out}, {"seq": far}),
        (z == half - 1, z == half, {"seq": z + 1}, {"seq": z - 1}),
        (core == 0, core == 1, {"fsdp": mate}, {"fsdp": mate}),
        (xpos == 0, xpos == 1, {"fsdp": xnbr}, {"fsdp": xnbr}),
        (ypos == 0, ypos == 1, {"fsdp": ynbr}, {"fsdp": ynbr}),
    )
    for below, _, child, _ in links:
        @pl.when(below)
        def _():
            pl.semaphore_signal(barrier, inc=1, device_id=child, device_id_type=MESH)

    parents = sum(jnp.where(above, 1, 0) for _, above, _, _ in links)

    @pl.when(parents > 0)
    def _():
        pl.semaphore_wait(barrier, parents)

    for i, (_, above, _, parent) in enumerate(links):
        @pl.when(above)
        def _():
            pl.semaphore_signal(ready.at[max(i - 1, 0)], inc=1, device_id=parent, device_id_type=MESH)

    def await_child(i):
        @pl.when(links[i][0])
        def _():
            pl.semaphore_wait(ready.at[max(i - 1, 0)], 1)

    def w_own(p):
        if p == 0:
            return wk_in
        if p == 1:
            return wv_in
        return wq_in.at[:, pl.ds((p - 2) * width, width)]

    def w_slot(p, f):
        return w.at[p, pl.ds(pl.multiple_of(f * depth, 16), depth), :]

    pair = pieces
    sets = pieces // pair

    def w_mark(p, kind, lane):
        if lane == 0:
            return w_recv.at[2 * sets + 1]
        return w_recv.at[(lane - 1) * sets + p // pair if kind == 0 else 2 * sets]

    def w_copy(p, kind, lane):
        shard = (me, xnbr, ynbr, diag)[kind]
        src = w_own(p) if kind == 0 else w_slot(p, shard)
        return pltpu.make_async_remote_copy(
            src_ref=src, dst_ref=w_slot(p, shard),
            send_sem=w_send.at[0], recv_sem=w_mark(p, kind, lane),
            device_id={"fsdp": (mate, xnbr, ynbr)[lane]}, device_id_type=MESH,
        )

    def w_wait(first, count, shard, sem):
        rows = pl.ds(pl.multiple_of(shard * depth, 16), depth)
        slots = w.at[pl.ds(first, count), rows, :]
        pltpu.make_async_copy(slots, slots, sem).wait()

    def w_bulk(count, sem):
        slots = w.at[:, pl.ds(0, count * depth), :]
        pltpu.make_async_copy(slots, slots, sem).wait()

    def t_slot(s, c):
        first = c * wire if isinstance(c, int) else pl.multiple_of(c * wire, wire)
        return tok.at[pl.ds(pl.multiple_of(s * cols, 16), cols), pl.ds(first, wire)]

    def t_pieces(block, c, side):
        if not isinstance(c, int) or c < chunks - 1:
            return [(t_slot(block, c), c)]
        early_at, late_at = (LATE, 0) if side == 0 else (0, cols - LATE)
        lanes = pl.ds(c * wire, wire)
        pieces_of = []
        for at, size, i in ((early_at, cols - LATE, c), (late_at, LATE, chunks)):
            rows = pl.ds(pl.multiple_of(block * cols + at, 16), size)
            pieces_of.append((tok.at[rows, lanes], i))
        return pieces_of

    def t_copies(block, c, side, direct=False, hop=0):
        return [
            pltpu.make_async_remote_copy(
                src_ref=tok_in.at[:, pl.ds(c * wire, wire)] if direct else ref, dst_ref=ref,
                send_sem=t_send.at[2 * hop + side], recv_sem=t_recv.at[block - side, i],
                device_id={"seq": z + 1 - 2 * side}, device_id_type=MESH,
            )
            for ref, i in t_pieces(block, c, side)
        ]

    def t_arrivals(block, c, side):
        def wait(ref, i):
            return lambda: pltpu.make_async_copy(ref, ref, t_recv.at[block - side, i]).wait()

        return [wait(ref, i) for ref, i in t_pieces(block, c, side)]

    def own_weights(do):
        for p in range(pieces):
            for lane in (1, 2, 0):
                do(w_copy(p, 0, lane))

    def start(copy):
        copy.start()

    def s_copy(block, side):
        return pltpu.make_async_remote_copy(
            src_ref=ss.at[block], dst_ref=ss.at[block],
            send_sem=s_send.at[0], recv_sem=s_recv.at[block - side],
            device_id={"seq": z + 1 - 2 * side}, device_id_type=MESH,
        )

    def s_wait(block, side):
        pltpu.make_async_copy(ss.at[block], ss.at[block], s_recv.at[block - side]).wait()

    def own_sums(do):
        @pl.when(z < n - 1)
        def _():
            do(s_copy(z, 0))

        @pl.when(z > 0)
        def _():
            do(s_copy(z, 1))

    def own_side(c, side, when, direct=False):
        @pl.when(when)
        def _():
            for copy in t_copies(z, c, side, direct):
                copy.start()

    def outward(c, when=True, direct=False):
        own_side(c, 1, ~outer & ~down & when, direct)
        own_side(c, 0, ~outer & down & when, direct)

    def inward(c, when=True):
        own_side(c, 0, ~down & when)
        own_side(c, 1, down & when)

    for c in range(AHEAD[0]):
        direct = c < DIRECT
        if not direct:
            for i in range(DIRECT + 1 if c == DIRECT else 0):
                loads[i].wait()
            if DIRECT < c < 3:
                loads[c].wait()
        outward(c, True if c < AHEAD[1] else core == 0, direct)
    for i in (2, 3, 4):
        await_child(i)
    own_weights(start)
    await_child(0)
    await_child(1)
    for c in range(INNER):
        inward(c)
    for c in range(INNER, chunks):
        inward(c, outer)
    local = []
    for p in range(pieces):
        local.append(pltpu.make_async_copy(w_own(p), w_slot(p, me), local_sem.at[0]))
    local.append(pltpu.make_async_copy(gain_in, gain_ref.at[0], local_sem.at[1]))
    local.append(pltpu.make_async_copy(trig_in, trig_ref, local_sem.at[2]))
    for copy in local:
        copy.start()
    v_s[:, :, HEAD_DIM:] = jnp.ones((kv, v_s.shape[1], HEAD_DIM), jnp.bfloat16)

    last = t_slot(z, chunks - 1)[...].astype(jnp.float32)
    ss[z] = jnp.sum(last * last, axis=0, keepdims=True)

    def relay(dist, c):
        @pl.when((z >= dist) & (z < n - 1))
        def _():
            for arrival, copy in zip(t_arrivals(z - dist, c, 0), t_copies(z - dist, c, 0, hop=dist)):
                arrival()
                copy.start()

        @pl.when((z + dist < n) & (z > 0))
        def _():
            for arrival, copy in zip(t_arrivals(z + dist, c, 1), t_copies(z + dist, c, 1, hop=dist)):
                arrival()
                copy.start()

    def relay_sums(dist):
        @pl.when((z >= dist) & (z < n - 1))
        def _():
            s_wait(z - dist, 0)
            s_copy(z - dist, 0).start()

        @pl.when((z + dist < n) & (z > 0))
        def _():
            s_wait(z + dist, 1)
            s_copy(z + dist, 1).start()

    def settle(dist, c, piece=0):
        @pl.when((z >= dist) & (z == n - 1))
        def _():
            t_arrivals(z - dist, c, 0)[piece]()

        @pl.when((z + dist < n) & (z == 0))
        def _():
            t_arrivals(z + dist, c, 1)[piece]()

    def token_round(k):
        for dist in range(n - 2, 0, -1):
            c = k - dist + 1
            if c == chunks - 1 and dist == 1:
                outward(c)
            if 0 <= c < chunks:
                relay(dist, c)
        for side_core in range(2):
            if k + AHEAD[side_core] < chunks - 1:
                outward(k + AHEAD[side_core], core == side_core)
        if k + INNER < chunks:
            inward(k + INNER, ~outer)

    rounds = chunks + n - 3
    early = min(n + 2, rounds)
    for step in range(max(early, pieces)):
        if step < early:
            token_round(step)
        if step == 2:
            own_sums(start)
        if 3 <= step <= n:
            relay_sums(step - 2)
        if step < pieces and step % pair == pair - 1:
            group = range(step + 1 - pair, step + 1)
            w_wait(group[0], pair, xnbr, w_recv.at[step // pair])
            for p in group:
                w_copy(p, 1, 0).start()

            @pl.when(core == 1)
            def _():
                for p in group:
                    w_copy(p, 1, 2).start()

            w_wait(group[0], pair, ynbr, w_recv.at[sets + step // pair])
            for p in group:
                w_copy(p, 2, 0).start()

            @pl.when(core == 0)
            def _():
                for p in group:
                    w_copy(p, 2, 1).start()

    w_wait(0, pieces, diag, w_recv.at[2 * sets])
    for p in range(pieces):
        w_copy(p, 3, 0).start()
    w_bulk(4, w_recv.at[2 * sets + 1])
    w_bulk(1, local_sem.at[0])
    for copy in local[pieces:]:
        copy.wait()

    scale = 1.0 / (12.0 * 50.0)
    peak = 50.0 * math.log2(math.e)

    R = wire

    def rotate_at(rows):
        cosine = trig_ref[0, rows, :]
        sine = trig_ref[1, rows, :]
        return lambda x: (x * cosine + pltpu.roll(x, HEAD_DIM // 2, 1) * sine).astype(jnp.bfloat16)

    def tail():
        length = chunks * wire
        first = length - R
        rows = pl.ds(first, R)
        near = (n - 1) * cols
        left = z == 0
        for dist in range(1, n):
            @pl.when(left)
            def _():
                s_wait(z + dist, 1)

            @pl.when(z == n - 1)
            def _():
                s_wait(z - dist, 0)

        for dist in range(1, n - 1):
            for piece in range(2):
                settle(dist, chunks - 1, piece)
        total = ss[0]
        for s in range(1, n):
            total += ss[s]
        inv = lax.rsqrt(total / (n * cols) + 1e-06)
        inv = jnp.broadcast_to(inv, (R, R)).T[:, :1]
        gain = gain_ref[...]
        some = cols - LATE
        spans = ((0, cols, near), (near, LATE, some), (near + some, 0, LATE))

        def normed(span):
            low, high, size = span
            at = pl.ds(pl.multiple_of(jnp.where(left, low, high), 16), size)
            scales = jnp.where(left, gain[:, low : low + size], gain[:, high : high + size])
            floats = tok[at, rows].T.astype(jnp.float32)
            return (floats * inv * scales).astype(jnp.bfloat16), at

        mine, at = normed(spans[0])
        for p in range(pieces):
            part_ref[p] = jnp.dot(mine, w[p, at, :], preferred_element_type=jnp.float32)
        settle(n - 1, chunks - 1, 0)
        mine, at = normed(spans[1])
        for p in range(pieces):
            part_ref[p] += jnp.dot(mine, w[p, at, :], preferred_element_type=jnp.float32)
        settle(n - 1, chunks - 1, 1)
        mine, at = normed(spans[2])
        turn = rotate_at(rows)

        def project(p):
            return part_ref[p] + jnp.dot(mine, w[p, at, :], preferred_element_type=jnp.float32)

        raw = project(0)
        for h in range(kv):
            k_s[h, rows, :] = turn(raw[:, h * HEAD_DIM : (h + 1) * HEAD_DIM])
        raw = project(1)
        for h in range(kv):
            v_s[h, rows, :HEAD_DIM] = raw[:, h * HEAD_DIM : (h + 1) * HEAD_DIM].astype(jnp.bfloat16)
        for g in range(groups):
            raw = project(2 + g)
            for i in range(kv):
                head = g * kv + i
                at_q = (head % groups) * R
                q_s[head // groups, at_q : at_q + R, :] = turn(raw[:, i * HEAD_DIM : (i + 1) * HEAD_DIM])

    def attend(rows, low, last, base_count):
        def block(h, keys, mask):
            s = lax.dot_general(
                q_s[h, : groups * R, :], k_s[h, keys, :], (((1,), (1,)), ((), ())),
                preferred_element_type=jnp.float32,
            )
            e = jnp.exp2(jnp.tanh(s * scale) * peak)
            if mask is not None:
                e = jnp.where(mask, e, 0.0)
            return jnp.dot(
                e.astype(jnp.bfloat16), v_s[h, keys, :], preferred_element_type=jnp.float32
            )

        row_id = lax.rem(lax.broadcasted_iota(jnp.int32, (groups * R, last), 0), R)
        mask = lax.broadcasted_iota(jnp.int32, (groups * R, last), 1) <= row_id + (last - R)
        top = pl.ds(low, last)
        for h in range(kv):
            acc[h, : groups * R, :] = block(h, top, mask)

        def inner(j, carry):
            keys = pl.ds(pl.multiple_of(j * ROWS, ROWS), ROWS)
            for h in range(kv):
                acc[h, : groups * R, :] += block(h, keys, None)
            return carry

        lax.fori_loop(0, base_count, inner, 0)
        for h in range(kv):
            for g in range(groups):
                sums = acc[h, g * R : (g + 1) * R, :]
                head = h * groups + g
                out_ref[rows, head * HEAD_DIM : (head + 1) * HEAD_DIM] = (
                    sums[:, :HEAD_DIM] / sums[:, HEAD_DIM:]
                ).astype(jnp.bfloat16)

    def chunk(first, low, last, base_count, part):
        rows = pl.ds(first, R)
        for dist in range(1, n):
            settle(dist, part)
        raw = tok[:, rows].T
        floats = raw.astype(jnp.float32)
        total = jnp.sum(floats * floats, axis=-1, keepdims=True)
        inv = lax.rsqrt(total / (n * cols) + 1e-06)
        nrm[:R, :] = (floats * inv * gain_ref[...]).astype(jnp.bfloat16)
        normed = nrm[:R, :]
        rotate = rotate_at(rows)

        raw = jnp.dot(normed, w[0], preferred_element_type=jnp.float32)
        for h in range(kv):
            k_s[h, rows, :] = rotate(raw[:, h * HEAD_DIM : (h + 1) * HEAD_DIM])
        raw = jnp.dot(normed, w[1], preferred_element_type=jnp.float32)
        for h in range(kv):
            v_s[h, rows, :HEAD_DIM] = raw[:, h * HEAD_DIM : (h + 1) * HEAD_DIM].astype(jnp.bfloat16)
        for g in range(groups):
            raw = jnp.dot(normed, w[2 + g], preferred_element_type=jnp.float32)
            for i in range(kv):
                head = g * kv + i
                at = (head % groups) * R
                q_s[head // groups, at : at + R, :] = rotate(
                    raw[:, i * HEAD_DIM : (i + 1) * HEAD_DIM]
                )

        @pl.when(part < chunks - 1)
        def _():
            attend(rows, low, last, base_count)

    def drain_tokens(block, side, hop=0):
        sent = tok.at[pl.ds(pl.multiple_of(block * cols, 16), cols), :]
        pltpu.make_async_copy(sent, sent, t_send.at[2 * hop + side]).wait()

    def drain_weights():
        @pl.when((z == 0) | (z == n - 1))
        def _():
            pltpu.make_async_copy(ss.at[pl.ds(0, 1)], ss.at[pl.ds(0, 1)], s_send.at[0]).wait()

        @pl.when((z > 0) & (z < n - 1))
        def _():
            sent = ss.at[pl.ds(0, n + 1)]
            pltpu.make_async_copy(sent, sent, s_send.at[0]).wait()

        w_bulk(7, w_send.at[0])

    def body(c, carry):
        @pl.when(c == 2)
        def _():
            drain_weights()

            @pl.when(z == 0)
            def _():
                drain_tokens(z, 0)

            @pl.when(z == n - 1)
            def _():
                drain_tokens(z, 1)

        low = pl.multiple_of(c * ROWS, ROWS)
        per = ROWS // R
        for i in range(per):
            first = pl.multiple_of(c * ROWS + i * R, R)
            part = c * per + i
            for k in range(early, rounds):
                before = 0 if k == early else FIRST + k - early - 1
                if before % per == i:
                    @pl.when(c == before // per)
                    def _():
                        token_round(k)

            if i < per - 1:
                chunk(first, low, (i + 1) * R, c, part)
            else:
                @pl.when((part < chunks - 1) | ((z > 0) & (z < n - 1)))
                def _():
                    chunk(first, low, (i + 1) * R, c, part)
        return carry

    lax.fori_loop(0, chunks * wire // ROWS, body, 0)

    @pl.when((z == 0) | (z == n - 1))
    def _():
        tail()

    @pl.when((z > 0) & (z < n - 1))
    def _():
        for side in range(2):
            drain_tokens(z, side)
        for dist in range(1, n - 1):
            @pl.when(z >= dist)
            def _():
                drain_tokens(z - dist, 0, dist)

            @pl.when(z + dist < n)
            def _():
                drain_tokens(z + dist, 1, dist)


def finish(out_ref, q_s, k_s, v_s, out_hbm, last_ref, sems):
    length, width = out_ref.shape
    kv, tall = q_s.shape[:2]
    groups = tall // WIRE
    R = WIRE
    first = length - R
    scale = 1.0 / (12.0 * 50.0)
    peak = 50.0 * math.log2(math.e)
    done = pl.ds(0, first)
    copies = [pltpu.make_async_copy(out_ref.at[done, :], out_hbm.at[done, :], sems.at[0])]
    copies[0].start()
    rows = pl.ds(first, R)
    row_id = lax.rem(lax.broadcasted_iota(jnp.int32, (groups * R, ROWS), 0), R)
    mask = lax.broadcasted_iota(jnp.int32, (groups * R, ROWS), 1) <= row_id + (ROWS - R)
    for h in range(kv):
        sums = None
        for low in range(length - ROWS, -1, -ROWS):
            keys = pl.ds(low, ROWS)
            s = lax.dot_general(
                q_s[h, : groups * R, :], k_s[h, keys, :], (((1,), (1,)), ((), ())),
                preferred_element_type=jnp.float32,
            )
            e = jnp.exp2(jnp.tanh(s * scale) * peak)
            if low + ROWS == length:
                e = jnp.where(mask, e, 0.0)
            e = jnp.dot(e.astype(jnp.bfloat16), v_s[h, keys, :], preferred_element_type=jnp.float32)
            sums = e if sums is None else sums + e
        for g in range(groups):
            head = h * groups + g
            part = sums[g * R : (g + 1) * R, :]
            last_ref[:, head * HEAD_DIM : (head + 1) * HEAD_DIM] = (
                part[:, :HEAD_DIM] / part[:, HEAD_DIM:]
            ).astype(jnp.bfloat16)
        lanes = pl.ds(h * groups * HEAD_DIM, groups * HEAD_DIM)
        copies.append(pltpu.make_async_copy(last_ref.at[:, lanes], out_hbm.at[rows, lanes], sems.at[1 + h]))
        copies[-1].start()
    for copy in copies:
        copy.wait()


def fused(n, fsdp, tokens, gain, w_query, w_key, w_value):
    length, cols = tokens.shape
    depth, width = w_key.shape
    kv = width // HEAD_DIM
    groups = w_query.shape[1] // width
    chunks = length // WIRE
    half = HEAD_DIM // 2
    freqs = 10000.0 ** (-2.0 * np.arange(half) / HEAD_DIM)
    angle = np.arange(length)[:, None] * freqs[None, :]
    cosine = np.concatenate([np.cos(angle)] * 2, axis=1).astype(np.float32)
    sine = np.concatenate([-np.sin(angle), np.sin(angle)], axis=1).astype(np.float32)
    hbm = pl.BlockSpec(memory_space=pl.ANY)
    pieces = 2 + groups
    flops = 2 * length * fsdp * depth * width * pieces
    vmem = pl.BlockSpec(memory_space=pltpu.VMEM)
    heads = w_query.shape[1]
    state = pl.pallas_call(
        functools.partial(kernel, n, kv, groups, chunks),
        out_shape=(
            pltpu.VMEM((length, heads), jnp.bfloat16),
            pltpu.VMEM((kv, groups * WIRE, HEAD_DIM), jnp.bfloat16),
            pltpu.VMEM((kv, length, HEAD_DIM), jnp.bfloat16),
            pltpu.VMEM((kv, length, 2 * HEAD_DIM), jnp.bfloat16),
        ),
        in_specs=[hbm] * 6,
        out_specs=[vmem] * 4,
        scratch_shapes=[
            pltpu.VMEM((n * cols, length), jnp.bfloat16),
            pltpu.VMEM((pieces, fsdp * depth, width), jnp.bfloat16),
            pltpu.VMEM((WIRE, n * cols), jnp.bfloat16),
            pltpu.VMEM((kv, groups * WIRE, 2 * HEAD_DIM), jnp.float32),
            pltpu.VMEM((1, n * cols), jnp.float32),
            pltpu.VMEM((2, length, HEAD_DIM), jnp.float32),
            pltpu.VMEM((pieces, WIRE, width), jnp.float32),
            pltpu.VMEM((n + 1, 1, WIRE), jnp.float32),
            pltpu.SemaphoreType.DMA((3,)),
            pltpu.SemaphoreType.DMA((3,)),
            pltpu.SemaphoreType.DMA((2 * (n - 1),)),
            pltpu.SemaphoreType.DMA((n - 1, chunks + 1)),
            pltpu.SemaphoreType.DMA((1,)),
            pltpu.SemaphoreType.DMA((4,)),
            pltpu.SemaphoreType.DMA((1,)),
            pltpu.SemaphoreType.DMA((n - 1,)),
            pltpu.SemaphoreType.REGULAR((4,)),
        ],
        compiler_params=pltpu.CompilerParams(
            collective_id=0, has_side_effects=True, vmem_limit_bytes=58 * 1024 * 1024
        ),
        cost_estimate=pl.CostEstimate(flops=flops, bytes_accessed=2 * length * cols, transcendentals=0),
    )(tokens.T, gain, jnp.asarray(np.stack([cosine, sine])), w_query, w_key, w_value)
    return pl.pallas_call(
        finish,
        out_shape=jax.ShapeDtypeStruct((length, heads), jnp.bfloat16),
        in_specs=[vmem] * 4,
        out_specs=hbm,
        scratch_shapes=[pltpu.VMEM((WIRE, heads), jnp.bfloat16), pltpu.SemaphoreType.DMA((1 + kv,))],
        compiler_params=pltpu.CompilerParams(vmem_limit_bytes=16 * 1024 * 1024),
    )(*(pltpu.with_memory_space_constraint(x, pltpu.VMEM) for x in state))


def rotate(values, positions):
    half = values.shape[-1] // 2
    index = jnp.arange(half, dtype=jnp.float32)
    freqs = jnp.power(jnp.float32(10000.0), -2.0 * index / values.shape[-1])
    angle = positions[:, None] * freqs[None, :]
    cosine = jnp.cos(angle)[:, None, :]
    sine = jnp.sin(angle)[:, None, :]
    first = values[..., :half]
    second = values[..., half:]
    return jnp.concatenate(
        [first * cosine - second * sine, second * cosine + first * sine], axis=-1
    )


def local(tokens, gain, w_query, w_key, w_value):
    features = gain.shape[0]
    floats = tokens.astype(jnp.float32)
    square_sum = lax.psum(jnp.sum(floats * floats, axis=-1), "seq")
    inv_rms = lax.rsqrt(square_sum / features + 1e-06)[:, None]
    own_cols = tokens.shape[1]
    gain_part = lax.dynamic_slice_in_dim(gain, lax.axis_index("seq") * own_cols, own_cols, 0)
    own_normed = (floats * inv_rms * gain_part[None, :]).astype(jnp.bfloat16)
    normed = lax.all_gather(own_normed, "seq", axis=1, tiled=True)
    length = normed.shape[0]

    def add_one(piece):
        return jnp.dot(normed, piece, preferred_element_type=jnp.float32)

    query_raw = add_one(lax.all_gather(w_query, "fsdp", axis=0, tiled=True))
    key_raw = add_one(lax.all_gather(w_key, "fsdp", axis=0, tiled=True))
    value_raw = add_one(lax.all_gather(w_value, "fsdp", axis=0, tiled=True))
    local_heads = w_query.shape[1] // HEAD_DIM
    local_kv = w_key.shape[1] // HEAD_DIM
    groups = local_heads // local_kv
    positions = jnp.arange(length, dtype=jnp.float32)
    values = value_raw.astype(jnp.bfloat16).reshape(length, local_kv, HEAD_DIM)
    query = rotate(query_raw.reshape(length, local_heads, HEAD_DIM), positions).astype(jnp.bfloat16)
    query = query.reshape(length, local_kv, groups, HEAD_DIM)
    keys = rotate(key_raw.reshape(length, local_kv, HEAD_DIM), positions).astype(jnp.bfloat16)
    scale = 1.0 / jnp.sqrt(jnp.float32(144.0))
    block_rows = 512
    outputs = []
    for first_row in range(0, length, block_rows):
        extent = first_row + block_rows
        query_block = query[first_row:extent]
        scores = (
            jnp.einsum(
                "lgqd,mgd->gqlm", query_block, keys[:extent], preferred_element_type=jnp.float32
            )
            * scale
        )
        capped = 50.0 * jnp.tanh(scores / 50.0)
        causal = jnp.arange(extent)[None, :] <= (first_row + jnp.arange(block_rows))[:, None]
        exponent = jnp.where(causal[None, None], jnp.exp(capped), 0.0)
        weights = (exponent / jnp.sum(exponent, axis=-1, keepdims=True)).astype(jnp.bfloat16)
        context = jnp.einsum(
            "gqlm,mgd->lgqd", weights, values[:extent], preferred_element_type=jnp.float32
        )
        outputs.append(context.reshape(block_rows, local_heads * HEAD_DIM).astype(jnp.bfloat16))
    return jnp.concatenate(outputs, axis=0)


def solution(mesh):
    n, fsdp = mesh.shape["seq"], mesh.shape["fsdp"]
    in_specs = (P("fsdp", "seq"), P(), P("fsdp", "seq"), P("fsdp", "seq"), P("fsdp", "seq"))
    out_specs = P("fsdp", "seq")

    def step(tokens, gain, w_query, w_key, w_value):
        fits = (
            fsdp == 8
            and n == 4
            and tokens.shape[1] % 16 == 0
            and tokens.shape[1] > LATE
            and tokens.shape[0] % ROWS == 0
            and tokens.shape[0] >= 3 * ROWS
            and w_key.shape[0] % 16 == 0
            and w_query.shape[1] % w_key.shape[1] == 0
        )
        if fits:
            return fused(n, fsdp, tokens, gain, w_query, w_key, w_value)
        return local(tokens, gain, w_query, w_key, w_value)

    return jax.shard_map(step, mesh=mesh, in_specs=in_specs, out_specs=out_specs, check_vma=False)
```
